128 devices in a mesh: batch: 1, k: 128 (over z, y, x, core).
Axes of the slice: x: 4, y: 4, z: 4, core: 2. Of those that a mesh axis runs over, the one named last changes fastest.
Arguments:
- a_vals: bfloat16 [128, 4, 128, 128], P(('batch', 'k'))
- b_vals: bfloat16 [128, 4, 128, 128], P(('batch', 'k'))
- pair_list: int32 [128, 4, 256, 2], P(('batch', 'k'))
- plist_idx: int32 [128, 256, 2], P(('batch', 'k'))
- c_idx: int32 [128, 16, 2], P(('batch', 'k'))
Outputs:
- output: float32 [128, 16, 128, 128], P(('batch', 'k'))
All inputs are finite; a program needn't handle non-finite values.
Results may differ from the reference program's by a relative error of at most 0.001.
Values are sent between devices in bfloat16 or wider.
A program may use at most 1 GiB of HBM per device.

```python
import jax
import jax.numpy as jnp
from jax import lax

KDEV = 128
NB = 181
OPS = 4
SEG = 2
MPAIR = 4
CAPC = 16
BLOCK = 128


def draw_layout(layout_key):
    key_rank, key_pick, key_mult, key_aslot, key_bslot, key_cells = jax.random.split(layout_key, 6)
    heavy_rank = jax.random.permutation(key_rank, KDEV)
    low_count = max(1, SEG // 4)
    counts = jnp.maximum(SEG // (1 + heavy_rank), low_count)
    cell_ids = jax.random.permutation(key_cells, NB * NB)[: KDEV * CAPC].reshape(KDEV, CAPC)
    c_idx = jnp.stack([cell_ids // NB, cell_ids % NB], axis=-1).astype(jnp.int32)
    scores = jax.random.randint(key_pick, (KDEV, KDEV, CAPC), 0, 1 << 20) * CAPC + jnp.arange(CAPC)
    chosen = jnp.argsort(scores, axis=-1)[:, :, :SEG]
    slot_used = jnp.arange(SEG)[None, None, :] < counts[:, None, None]
    coords = c_idx[jnp.arange(KDEV)[None, :, None], chosen]
    plist_idx = jnp.where(slot_used[..., None], coords, -1).reshape(KDEV, KDEV * SEG, 2)
    pair_mult = 1 + jax.random.randint(key_mult, (KDEV, KDEV, SEG), 0, MPAIR) // (1 + heavy_rank[:, None, None])
    active = slot_used[:, None] & (jnp.arange(MPAIR)[None, :, None, None] < pair_mult[:, None])
    a_slot = jax.random.randint(key_aslot, (KDEV, MPAIR, KDEV, SEG), 0, OPS)
    b_slot = jax.random.randint(key_bslot, (KDEV, MPAIR, KDEV, SEG), 0, OPS)
    pair_list = jnp.where(active[..., None], jnp.stack([a_slot, b_slot], axis=-1), -1)
    pair_list = pair_list.reshape(KDEV, MPAIR, KDEV * SEG, 2).astype(jnp.int32)
    return pair_list, plist_idx.astype(jnp.int32), c_idx


def setup_inputs(seed: int = 0, part: int = 0) -> dict:
    base_key = jax.random.fold_in(jax.random.key(seed), part)
    key_layout, key_a, key_b = jax.random.split(base_key, 3)
    pair_list, plist_idx, c_idx = draw_layout(key_layout)
    a_vals = (jax.random.normal(key_a, (KDEV, OPS, BLOCK, BLOCK), jnp.float32) * BLOCK ** -0.5).astype(jnp.bfloat16)
    b_vals = jax.random.normal(key_b, (KDEV, OPS, BLOCK, BLOCK), jnp.float32).astype(jnp.bfloat16)
    return {"a_vals": a_vals, "b_vals": b_vals, "pair_list": pair_list, "plist_idx": plist_idx, "c_idx": c_idx}


def reference(a_vals, b_vals, pair_list, plist_idx, c_idx):
    a_flat = a_vals.reshape(KDEV * OPS, BLOCK, BLOCK)
    b_flat = b_vals.reshape(KDEV * OPS, BLOCK, BLOCK)
    row_base = (jnp.arange(KDEV) * OPS)[:, None]

    def owner_blocks(owner_id):
        seg_pairs = lax.dynamic_slice_in_dim(pair_list, owner_id * SEG, SEG, axis=2)
        seg_coords = lax.dynamic_slice_in_dim(plist_idx, owner_id * SEG, SEG, axis=1).reshape(KDEV * SEG, 2)

        def pair_step(running, pair_rank):
            is_pair = pair_rank[..., 0] >= 0
            left_ops = a_flat[row_base + jnp.maximum(pair_rank[..., 0], 0)].astype(jnp.float32)
            right_ops = b_flat[row_base + jnp.maximum(pair_rank[..., 1], 0)].astype(jnp.float32)
            product = jnp.einsum("psab,psbc->psac", left_ops, right_ops)
            return running + jnp.where(is_pair[..., None, None], product, 0.0), None

        start_acc = jnp.zeros((KDEV, SEG, BLOCK, BLOCK), jnp.float32)
        scan_out = lax.scan(pair_step, start_acc, jnp.moveaxis(seg_pairs, 1, 0))
        sent_blocks = scan_out[0].astype(jnp.bfloat16).astype(jnp.float32).reshape(KDEV * SEG, BLOCK, BLOCK)
        owned_idx = c_idx[owner_id]
        matched = ((seg_coords[None, :, 0] == owned_idx[:, None, 0]) & (seg_coords[None, :, 1] == owned_idx[:, None, 1]) & (seg_coords[None, :, 0] >= 0))
        return jnp.einsum("tr,rac->tac", matched.astype(jnp.float32), sent_blocks)

    return lax.map(owner_blocks, jnp.arange(KDEV))
```

```python
import functools

import jax
import jax.numpy as jnp
from jax import lax
from jax.experimental import pallas as pl
from jax.experimental.pallas import tpu as pltpu
from jax.sharding import PartitionSpec as P

RING = 4
SIDE = 4
PLANE = 32
LINES = PLANE // 2
SLOTS = 8
NOPAIR = 16
NOSLOT = PLANE * SLOTS


def order_of(j):
    return j + (j // 2) * (1 - 2 * (j % 2))


def kernel(a_ref, b_ref, tbl_ref, crow_ref, out_ref, held, prod0, prod1, parts, acc, opp, fin, tblb, cb, selv,
           tbl_s, sel_s, local_sem, own_sem, sib_sem, f_sem, s_sem, d_sem, tsend_sem, trecv_sem, csend_sem, crecv_sem,
           tloc_sem, smem_sem, sel_sem, rs_send, opp_sem, fin_sem):
    me = lax.axis_index("k")
    z = me // PLANE
    d = me % PLANE
    y = d // 8
    x = (d // 2) % 4
    c = d % 2
    n_own = out_ref.shape[0]
    half_own = n_own // 2

    def dev(zz, yy, xx, cc):
        return {"k": ((zz * 4 + yy) * 4 + xx) * 2 + cc}

    sibling = dev(z, y, x, 1 - c)

    def f_dev(off):
        return dev(z, (y + off * c) % 4, (x + off * (1 - c)) % 4, c)

    def s_dev(off):
        return dev(z, (y + off * (1 - c)) % 4, (x + off * c) % 4, c)

    def z_dev(off):
        return {"k": ((z + off) % 4) * PLANE + d}

    def slot_of(core, df, ds):
        sx = (x + df * (1 - core) + ds * core) % 4
        sy = (y + df * core + ds * (1 - core)) % 4
        return sy * 4 + sx

    barrier = pltpu.get_barrier_semaphore()

    def greet(r, carry):
        pl.semaphore_signal(barrier, inc=1, device_id={"k": z * PLANE + (d + r) % PLANE},
                            device_id_type=pl.DeviceIdType.MESH)
        return carry

    lax.fori_loop(1, PLANE, greet, 0)
    for off in (1, 2, 3):
        pl.semaphore_signal(barrier, inc=1, device_id=z_dev(off), device_id_type=pl.DeviceIdType.MESH)

    my_slot = y * 4 + x

    def half(core, slot, h):
        return held.at[core, slot, pl.ds(4 * h, 4)]

    loads = [
        pltpu.make_async_copy(ref.at[pl.ds(2 * h, 2)], held.at[c, my_slot, pl.ds(4 * h + 2 * w, 2)],
                              local_sem.at[2 * h + w])
        for h in (0, 1) for w, ref in enumerate((a_ref, b_ref))
    ]
    for cp in loads:
        cp.start()
    tloc = pltpu.make_async_copy(tbl_ref.at[pl.ds(2 * d, 2)], tblb.at[pl.ds(2 * d, 2)], tloc_sem.at[0])
    cloc = pltpu.make_async_copy(crow_ref, cb.at[pl.ds(z, 1)], tloc_sem.at[1])
    tloc.start()
    cloc.start()

    zero = jnp.zeros(prod0.shape[1:], jnp.float32)
    prod0[NOPAIR] = zero
    prod1[NOPAIR] = zero
    parts[NOSLOT] = zero

    pl.semaphore_wait(barrier, PLANE - 1 + 3)

    def push(core, slot, h, target, send_sem, recv):
        pltpu.make_async_remote_copy(
            src_ref=half(core, slot, h), dst_ref=half(core, slot, h), send_sem=send_sem,
            recv_sem=recv.at[slot, h], device_id=target, device_id_type=pl.DeviceIdType.MESH).start()

    def arrived(core, slot, h, recv):
        pltpu.make_async_copy(half(core, slot, h), half(core, slot, h), recv.at[slot, h]).wait()

    def to_sibling(slot, h):
        push(c, slot, h, sibling, d_sem.at[0], sib_sem)

    for cp in loads:
        cp.wait()
    for h in (0, 1):
        for off in (1, 3):
            push(c, my_slot, h, f_dev(off), f_sem.at[0], own_sem)
            push(c, my_slot, h, s_dev(off), s_sem.at[0], own_sem)
        to_sibling(my_slot, h)

    def send_tables(r, carry):
        peer = (d + r) % PLANE
        pltpu.make_async_remote_copy(
            src_ref=tbl_ref.at[pl.ds(2 * peer, 2)], dst_ref=tblb.at[pl.ds(2 * d, 2)], send_sem=tsend_sem.at[0],
            recv_sem=trecv_sem.at[0], device_id={"k": z * PLANE + peer},
            device_id_type=pl.DeviceIdType.MESH).start()
        return carry

    lax.fori_loop(1, PLANE, send_tables, 0)
    for off in (1, 2, 3):
        pltpu.make_async_remote_copy(
            src_ref=crow_ref, dst_ref=cb.at[pl.ds(z, 1)], send_sem=csend_sem.at[0], recv_sem=crecv_sem.at[0],
            device_id=z_dev(off), device_id_type=pl.DeviceIdType.MESH).start()

    def bytes_wait(ref, sem):
        pltpu.make_async_copy(ref, ref, sem).wait()

    tloc.wait()
    cloc.wait()
    bytes_wait(tblb.at[pl.ds(0, 2 * (PLANE - 1))], trecv_sem.at[0])
    bytes_wait(cb.at[pl.ds(0, 3)], crecv_sem.at[0])
    to_smem = pltpu.make_async_copy(tblb, tbl_s, smem_sem.at[0])
    to_smem.start()
    codes = jnp.concatenate([tblb[pl.ds(2 * p + 1, 1), 0] for p in range(PLANE)], axis=0)
    wanted = jnp.sum(cb[...], axis=0)
    row = lax.broadcasted_iota(jnp.int32, codes.shape, 0)
    lane = lax.broadcasted_iota(jnp.int32, codes.shape, 1)
    index = row * SLOTS + 2 * ((lane % 64) // n_own) + lane // 64
    hit = jnp.where(codes == wanted, index - NOSLOT, 0)
    selv[...] = NOSLOT + jnp.where(hit != 0, hit, pltpu.roll(hit, 64, 1))
    to_smem.wait()

    def compute(core, slot, prod):
        lhs = jnp.concatenate([held[core, slot, i] for i in (0, 1, 4, 5)], axis=0)
        rows = lhs.shape[0] // 4
        cols = held.shape[-1]
        for pair in (0, 1):
            rhs = jnp.concatenate([held[core, slot, 2 + 4 * pair], held[core, slot, 3 + 4 * pair]], axis=1)
            res = jnp.dot(lhs, rhs, preferred_element_type=jnp.float32)
            for a in range(4):
                for b in (0, 1):
                    prod[a * 4 + 2 * pair + b] = res[a * rows:(a + 1) * rows, b * cols:(b + 1) * cols]
        src = slot * 2 + core
        for j in range(SLOTS):
            total = prod[tbl_s[2 * src, 0, 4 * j]]
            for u in (1, 2, 3):
                total = total + prod[tbl_s[2 * src, 0, 4 * j + u]]
            parts[src * SLOTS + j] = total.astype(jnp.bfloat16).astype(jnp.float32)

    def both(df, ds):
        slot = slot_of(1 - c, df, ds)
        for h in (0, 1):
            arrived(1 - c, slot, h, sib_sem)
        compute(c, slot_of(c, df, ds), prod0)
        compute(1 - c, slot, prod1)

    both(0, 0)
    to_sel = pltpu.make_async_copy(selv, sel_s, sel_sem.at[0])
    to_sel.start()

    def first_line(j, carry):
        df = order_of(j)
        slot = slot_of(c, df, 0)
        for h in (0, 1):
            arrived(c, slot, h, own_sem)
            if h == 0:
                @pl.when(df == 3)
                def _():
                    push(c, slot, 0, f_dev(1), f_sem.at[0], own_sem)
            else:
                @pl.when(df == 1)
                def _():
                    push(c, slot, 1, f_dev(3), f_sem.at[0], own_sem)
            for off in (1, 3):
                push(c, slot, h, s_dev(off), s_sem.at[0], own_sem)
            to_sibling(slot, h)
        both(df, 0)
        return carry

    lax.fori_loop(1, 4, first_line, 0)

    def neighbours(k, carry):
        df = order_of(k // 2)
        ds = 1 + 2 * (k % 2)
        slot = slot_of(c, df, ds)
        for h in (0, 1):
            arrived(c, slot, h, own_sem)
            if h == 0:
                @pl.when(ds == 3)
                def _():
                    push(c, slot, 0, s_dev(1), s_sem.at[0], own_sem)
            else:
                @pl.when(ds == 1)
                def _():
                    push(c, slot, 1, s_dev(3), s_sem.at[0], own_sem)
            to_sibling(slot, h)
        both(df, ds)
        return carry

    lax.fori_loop(0, 8, neighbours, 0)

    def opposite(j, carry):
        df = order_of(j)
        slot = slot_of(c, df, 2)
        for h in (0, 1):
            arrived(c, slot, h, own_sem)
            to_sibling(slot, h)
        both(df, 2)
        return carry

    lax.fori_loop(0, 4, opposite, 0)
    to_sel.wait()

    def block_sum(zz, t):
        def add(p4, total):
            for u in range(8):
                total = total + parts[sel_s[p4 * 8 + u, zz * n_own + t]]
            return total
        return lax.fori_loop(0, PLANE // 8, add, zero)

    def z_push(rel, t, dst, recv, off):
        zz = (z + rel) % 4
        pltpu.make_async_remote_copy(
            src_ref=acc.at[zz, t], dst_ref=dst, send_sem=rs_send.at[0], recv_sem=recv, device_id=z_dev(off),
            device_id_type=pl.DeviceIdType.MESH).start()

    z_up, z_two, z_down = (z + 1) % 4, (z + 2) % 4, (z + 3) % 4

    def far(t, carry):
        acc[z_two, t] = block_sum(z_two, t)
        acc[z_two, t + half_own] = block_sum(z_two, t + half_own)
        z_push(2, t, opp.at[0, t], opp_sem.at[0, t], 1)
        z_push(2, t + half_own, opp.at[1, t], opp_sem.at[1, t], 3)
        return carry

    lax.fori_loop(0, half_own, far, 0)

    def near(t, carry):
        acc[z_up, t + half_own] = block_sum(z_up, t + half_own)
        acc[z_down, t] = block_sum(z_down, t)
        z_push(1, t + half_own, fin.at[0, t + half_own], fin_sem.at[0, t + half_own], 1)
        z_push(3, t, fin.at[1, t], fin_sem.at[1, t], 3)
        return carry

    lax.fori_loop(0, half_own, near, 0)

    def combined(t, carry):
        up = block_sum(z_up, t)
        down = block_sum(z_down, t + half_own)
        bytes_wait(opp.at[0, t], opp_sem.at[0, t])
        bytes_wait(opp.at[1, t], opp_sem.at[1, t])
        acc[z_up, t] = up + opp[0, t]
        acc[z_down, t + half_own] = down + opp[1, t]
        z_push(1, t, fin.at[0, t], fin_sem.at[0, t], 1)
        z_push(3, t + half_own, fin.at[1, t + half_own], fin_sem.at[1, t + half_own], 3)
        return carry

    lax.fori_loop(0, half_own, combined, 0)

    def mine(t, carry):
        acc[z, t] = block_sum(z, t)
        return carry

    lax.fori_loop(0, n_own, mine, 0)

    def finish(t, carry):
        for tt in (t, t + half_own):
            bytes_wait(fin.at[0, tt], fin_sem.at[0, tt])
            bytes_wait(fin.at[1, tt], fin_sem.at[1, tt])
            out_ref[tt] = acc[z, tt] + (fin[0, tt] + fin[1, tt])
        return carry

    lax.fori_loop(0, half_own, finish, 0)

    bytes_wait(held.at[0, pl.ds(0, 3)], f_sem.at[0])
    bytes_wait(held.at[0, pl.ds(0, 12)], s_sem.at[0])
    bytes_wait(held.at[0], d_sem.at[0])
    bytes_wait(tblb.at[pl.ds(0, 2 * (PLANE - 1))], tsend_sem.at[0])
    bytes_wait(cb.at[pl.ds(0, 3)], csend_sem.at[0])
    bytes_wait(acc.at[pl.ds(0, 3)], rs_send.at[0])


def tables(pairs, coords, cidx, z):
    n_own = cidx.shape[0]
    pid = jnp.where(pairs[..., 0] >= 0, pairs[..., 0] * 4 + pairs[..., 1], NOPAIR)
    pid = pid.reshape(4, RING, PLANE, 2).transpose(2, 1, 3, 0).reshape(PLANE, 1, 4 * SLOTS)
    pid = jnp.pad(pid, ((0, 0), (0, 0), (0, 128 - 4 * SLOTS)))
    code = jnp.where(coords[:, 0] >= 0, coords[:, 0] * 256 + coords[:, 1], -1)
    code = code.reshape(RING, PLANE, 2).transpose(1, 2, 0)
    code = jnp.broadcast_to(code[..., None], (PLANE, 2, RING, n_own)).reshape(PLANE, 1, 128)
    tbl = jnp.concatenate([pid, code], axis=1).reshape(2 * PLANE, 1, 128)
    own = cidx[:, 0] * 256 + cidx[:, 1]
    at = jnp.arange(RING)[:, None] == z
    crow = jnp.broadcast_to(jnp.where(at, own[None, :], 0)[None], (2, RING, n_own)).reshape(1, 1, 128)
    return tbl, crow


def solution(mesh):
    dev_spec = P(("batch", "k"))

    def per_device(a_loc, b_loc, pair_loc, coord_loc, cidx_loc):
        a, b, cidx = a_loc[0], b_loc[0], cidx_loc[0]
        n_own = cidx.shape[0]
        rows, cols = a.shape[1], b.shape[2]
        tbl, crow = tables(pair_loc[0], coord_loc[0], cidx, lax.axis_index("k") // PLANE)
        blk = (rows, cols)
        f32, i32 = jnp.float32, jnp.int32
        dma = pltpu.SemaphoreType.DMA
        out = pl.pallas_call(
            kernel,
            out_shape=jax.ShapeDtypeStruct((n_own,) + blk, f32),
            in_specs=[pl.BlockSpec(memory_space=pl.ANY)] * 4,
            out_specs=pl.BlockSpec(memory_space=pltpu.VMEM),
            scratch_shapes=[
                pltpu.VMEM((2, LINES, 8) + blk, jnp.bfloat16),
                pltpu.VMEM((NOPAIR + 1,) + blk, f32),
                pltpu.VMEM((NOPAIR + 1,) + blk, f32),
                pltpu.VMEM((NOSLOT + 1,) + blk, f32),
                pltpu.VMEM((RING, n_own) + blk, f32),
                pltpu.VMEM((2, n_own // 2) + blk, f32),
                pltpu.VMEM((2, n_own) + blk, f32),
                pltpu.VMEM((2 * PLANE, 1, 128), i32),
                pltpu.VMEM((RING, 1, 128), i32),
                pltpu.VMEM((PLANE, 128), i32),
                pltpu.SMEM((2 * PLANE, 1, 128), i32),
                pltpu.SMEM((PLANE, 128), i32),
                dma((4,)), dma((LINES, 2)), dma((LINES, 2)), dma((1,)), dma((1,)), dma((1,)), dma((1,)), dma((1,)),
                dma((1,)), dma((1,)), dma((2,)), dma((1,)), dma((1,)), dma((1,)), dma((2, n_own // 2)),
                dma((2, n_own)),
            ],
            compiler_params=pltpu.CompilerParams(collective_id=0, has_side_effects=True,
                                                 vmem_limit_bytes=60 * 1024 * 1024),
        )(a, b, tbl, crow)
        return out[None]

    return jax.shard_map(per_device, mesh=mesh, in_specs=(dev_spec,) * 5, out_specs=dev_spec, check_vma=False)
```

```python
import jax
import jax.numpy as jnp
from jax import lax
from jax.experimental import pallas as pl
from jax.experimental.pallas import tpu as pltpu
from jax.sharding import PartitionSpec as P

RING = 4
PLANE = 32
LINES = PLANE // 2
SLOTS = 8
NOPAIR = 16
NOSLOT = PLANE * SLOTS
CHUNKS = 2
GROUP = 2
MESH = pl.DeviceIdType.MESH


def order_of(j):
    return j + (j // 2) * (1 - 2 * (j % 2))


def kernel(a_ref, b_ref, tbl_ref, crow_ref, out_ref, held_b, held_a, prods, parts, acc, opp, fin, tblb, cb, selv,
           tbl_s, sel_s, local_sem, own_sem, sib_sem, f_sem, s_sem, d_sem, tsend_sem, trecv_sem, csend_sem, crecv_sem,
           tloc_sem, smem_sem, sel_sem, rs_send, opp_sem, fin_sem):
    me = lax.axis_index("k")
    z = me // PLANE
    d = me % PLANE
    y = d // 8
    x = (d // 2) % 4
    c = d % 2
    n_own = out_ref.shape[0]
    half_own = n_own // 2
    n_grp = half_own // GROUP
    chunk_rows = out_ref.shape[1] // CHUNKS
    cols = out_ref.shape[2]

    def dev(zz, yy, xx, cc):
        return {"k": ((zz * 4 + yy) * 4 + xx) * 2 + cc}

    sibling = dev(z, y, x, 1 - c)

    def f_dev(off):
        return dev(z, (y + off * c) % 4, (x + off * (1 - c)) % 4, c)

    def s_dev(off):
        return dev(z, (y + off * (1 - c)) % 4, (x + off * c) % 4, c)

    def z_dev(off):
        return {"k": ((z + off) % 4) * PLANE + d}

    def slot_of(core, df, ds):
        sx = (x + df * (1 - core) + ds * core) % 4
        sy = (y + df * core + ds * (1 - core)) % 4
        return sy * 4 + sx

    barrier = pltpu.get_barrier_semaphore()

    def greet(r, carry):
        pl.semaphore_signal(barrier, inc=1, device_id={"k": z * PLANE + (d + r) % PLANE}, device_id_type=MESH)
        return carry

    lax.fori_loop(1, PLANE, greet, 0)
    for off in (1, 2, 3):
        pl.semaphore_signal(barrier, inc=1, device_id=z_dev(off), device_id_type=MESH)

    my_slot = y * 4 + x
    pieces = [held_b] + list(held_a)

    loads = [pltpu.make_async_copy(b_ref, held_b.at[c, my_slot], local_sem.at[0])]
    for ch in range(CHUNKS):
        loads.append(pltpu.make_async_copy(a_ref.at[:, pl.ds(ch * chunk_rows, chunk_rows)], held_a[ch].at[c, my_slot],
                                           local_sem.at[1 + ch]))
    for cp in loads:
        cp.start()
    tloc = pltpu.make_async_copy(tbl_ref.at[pl.ds(2 * d, 2)], tblb.at[pl.ds(2 * d, 2)], tloc_sem.at[0])
    cloc = pltpu.make_async_copy(crow_ref, cb.at[pl.ds(z, 1)], tloc_sem.at[1])
    tloc.start()
    cloc.start()

    zero = jnp.zeros((chunk_rows, cols), jnp.float32)
    for ref in prods:
        ref[NOPAIR] = zero
    for ref in parts:
        ref[NOSLOT] = zero

    pl.semaphore_wait(barrier, PLANE - 1 + 3)

    def whole(k, core, slot):
        return pieces[k].at[core, slot]

    def half(k, core, slot, h):
        return pieces[k].at[core, slot, pl.ds(2 * h, 2)]

    def send(ref, target, send_sem, recv_sem):
        pltpu.make_async_remote_copy(src_ref=ref, dst_ref=ref, send_sem=send_sem, recv_sem=recv_sem,
                                     device_id=target, device_id_type=MESH).start()

    def bytes_wait(ref, sem):
        pltpu.make_async_copy(ref, ref, sem).wait()

    def to_sibling(k, slot):
        send(whole(k, c, slot), sibling, d_sem.at[k], sib_sem.at[k, slot])

    def to_f(k, slot):
        for off in (1, 3):
            send(whole(k, c, slot), f_dev(off), f_sem.at[k], own_sem.at[k, slot, 0])

    def to_s(k, slot):
        for off in (1, 3):
            send(whole(k, c, slot), s_dev(off), s_sem.at[k], own_sem.at[k, slot, 0])

    def got_whole(k, slot):
        bytes_wait(whole(k, c, slot), own_sem.at[k, slot, 0])

    def got_halves(k, slot):
        for h in (0, 1):
            bytes_wait(half(k, c, slot, h), own_sem.at[k, slot, h])

    def line_near(k):
        for df, h, off in ((1, 1, 3), (3, 0, 1)):
            slot = slot_of(c, df, 0)
            got_whole(k, slot)
            send(half(k, c, slot, h), f_dev(off), f_sem.at[k], own_sem.at[k, slot, h])
            to_s(k, slot)
            to_sibling(k, slot)

    def line_far(k):
        slot = slot_of(c, 2, 0)
        got_halves(k, slot)
        to_s(k, slot)
        to_sibling(k, slot)

    def side_near(k, df):
        for ds, h, off in ((1, 1, 3), (3, 0, 1)):
            slot = slot_of(c, df, ds)
            got_whole(k, slot)
            send(half(k, c, slot, h), s_dev(off), s_sem.at[k], own_sem.at[k, slot, h])
            to_sibling(k, slot)

    def side_far(k, df):
        slot = slot_of(c, df, 2)
        got_halves(k, slot)
        to_sibling(k, slot)

    for k in range(1 + CHUNKS):
        loads[k].wait()
        to_f(k, my_slot)
        if k < 2:
            to_s(k, my_slot)
            to_sibling(k, my_slot)

    def send_tables(r, carry):
        peer = (d + r) % PLANE
        pltpu.make_async_remote_copy(
            src_ref=tbl_ref.at[pl.ds(2 * peer, 2)], dst_ref=tblb.at[pl.ds(2 * d, 2)], send_sem=tsend_sem.at[0],
            recv_sem=trecv_sem.at[0], device_id={"k": z * PLANE + peer}, device_id_type=MESH).start()
        return carry

    lax.fori_loop(1, PLANE, send_tables, 0)
    for off in (1, 2, 3):
        pltpu.make_async_remote_copy(
            src_ref=crow_ref, dst_ref=cb.at[pl.ds(z, 1)], send_sem=csend_sem.at[0], recv_sem=crecv_sem.at[0],
            device_id=z_dev(off), device_id_type=MESH).start()

    line_near(0)
    side_near(0, 0)
    line_near(1)
    line_far(0)

    tloc.wait()
    cloc.wait()
    bytes_wait(tblb.at[pl.ds(0, 2 * (PLANE - 1))], trecv_sem.at[0])
    bytes_wait(cb.at[pl.ds(0, 3)], crecv_sem.at[0])
    to_smem = pltpu.make_async_copy(tblb, tbl_s, smem_sem.at[0])
    to_smem.start()

    side_near(0, 1)
    side_near(0, 3)
    line_far(1)

    codes = jnp.concatenate([tblb[pl.ds(2 * p + 1, 1), 0] for p in range(PLANE)], axis=0)
    wanted = jnp.sum(cb[...], axis=0)
    row = lax.broadcasted_iota(jnp.int32, codes.shape, 0)
    lane = lax.broadcasted_iota(jnp.int32, codes.shape, 1)
    index = row * SLOTS + 2 * ((lane % 64) // n_own) + lane // 64
    hit = jnp.where(codes == wanted, index - NOSLOT, 0)
    selv[...] = NOSLOT + jnp.where(hit != 0, hit, pltpu.roll(hit, 64, 1))

    side_near(0, 2)
    for j in range(4):
        side_far(0, order_of(j))
    to_smem.wait()
    to_sel = pltpu.make_async_copy(selv, sel_s, sel_sem.at[0])
    to_sel.start()

    def compute(ch, core, df, ds, prod):
        slot = slot_of(core, df, ds)
        lhs = held_a[ch][core, slot].reshape(4 * chunk_rows, -1)
        for pair in (0, 1):
            rhs = jnp.concatenate([held_b[core, slot, 2 * pair], held_b[core, slot, 2 * pair + 1]], axis=1)
            res = jnp.dot(lhs, rhs, preferred_element_type=jnp.float32)
            for a in range(4):
                for b in (0, 1):
                    prod[a * 4 + 2 * pair + b] = res[a * chunk_rows:(a + 1) * chunk_rows, b * cols:(b + 1) * cols]
        src = slot * 2 + core
        for j in range(SLOTS):
            total = prod[tbl_s[2 * src, 0, 4 * j]]
            for u in (1, 2, 3):
                total = total + prod[tbl_s[2 * src, 0, 4 * j + u]]
            parts[ch][src * SLOTS + j] = total.astype(jnp.bfloat16).astype(jnp.float32)

    def both(ch, df, ds, first=True):
        slot = slot_of(1 - c, df, ds)
        if ch == 0:
            bytes_wait(whole(0, 1 - c, slot), sib_sem.at[0, slot])
        bytes_wait(whole(1 + ch, 1 - c, slot), sib_sem.at[1 + ch, slot])
        compute(ch, c, df, ds, prods[0])
        compute(ch, 1 - c, df, ds, prods[1])

    def loop(n, body):
        def run(j, carry):
            body(j)
            return carry
        lax.fori_loop(0, n, run, 0)

    def block_sum(ch, zz, t):
        def add(p8, total):
            for u in range(8):
                total = total + parts[ch][sel_s[p8 * 8 + u, zz * n_own + t]]
            return total
        return lax.fori_loop(0, PLANE // 8, add, zero)

    z_up, z_two, z_down = (z + 1) % 4, (z + 2) % 4, (z + 3) % 4

    def z_push(ch, zz, t, dst, recv, off):
        pltpu.make_async_remote_copy(
            src_ref=acc[ch].at[zz, pl.ds(t, GROUP)], dst_ref=dst, send_sem=rs_send.at[ch], recv_sem=recv,
            device_id=z_dev(off), device_id_type=MESH).start()

    def far(ch):
        def body(g):
            t = g * GROUP
            for u in range(GROUP):
                acc[ch][z_two, t + u] = block_sum(ch, z_two, t + u)
                acc[ch][z_two, t + half_own + u] = block_sum(ch, z_two, t + half_own + u)
            z_push(ch, z_two, t, opp[ch].at[0, pl.ds(t, GROUP)], opp_sem.at[ch, 0, g], 1)
            z_push(ch, z_two, t + half_own, opp[ch].at[1, pl.ds(t, GROUP)], opp_sem.at[ch, 1, g], 3)
        loop(n_grp, body)

    def near(ch):
        def body(g):
            t = g * GROUP
            for u in range(GROUP):
                acc[ch][z_up, t + half_own + u] = block_sum(ch, z_up, t + half_own + u)
                acc[ch][z_down, t + u] = block_sum(ch, z_down, t + u)
            z_push(ch, z_up, t + half_own, fin[ch].at[0, pl.ds(t + half_own, GROUP)], fin_sem.at[ch, 0, g + n_grp], 1)
            z_push(ch, z_down, t, fin[ch].at[1, pl.ds(t, GROUP)], fin_sem.at[ch, 1, g], 3)
        loop(n_grp, body)

    def combined(ch):
        def body(g):
            t = g * GROUP
            up = [block_sum(ch, z_up, t + u) for u in range(GROUP)]
            for u in range(GROUP):
                acc[ch][z_up, t + u] = up[u]
            down = [block_sum(ch, z_down, t + half_own + u) for u in range(GROUP)]
            for u in range(GROUP):
                acc[ch][z_down, t + half_own + u] = down[u]
            bytes_wait(opp[ch].at[0, pl.ds(t, GROUP)], opp_sem.at[ch, 0, g])
            bytes_wait(opp[ch].at[1, pl.ds(t, GROUP)], opp_sem.at[ch, 1, g])
            for u in range(GROUP):
                acc[ch][z_up, t + u] += opp[ch][0, t + u]
                acc[ch][z_down, t + half_own + u] += opp[ch][1, t + u]
            z_push(ch, z_up, t, fin[ch].at[0, pl.ds(t, GROUP)], fin_sem.at[ch, 0, g], 1)
            z_push(ch, z_down, t + half_own, fin[ch].at[1, pl.ds(t + half_own, GROUP)], fin_sem.at[ch, 1, g + n_grp], 3)
        loop(n_grp, body)

    def mine(ch):
        def body(t):
            acc[ch][z, t] = block_sum(ch, z, t)
        loop(n_own, body)

    def finish(ch):
        def body(g):
            for gg in (g, g + n_grp):
                t = gg * GROUP
                for side in (0, 1):
                    bytes_wait(fin[ch].at[side, pl.ds(t, GROUP)], fin_sem.at[ch, side, gg])
                for u in range(GROUP):
                    out_ref[t + u, pl.ds(ch * chunk_rows, chunk_rows)] = (
                        acc[ch][z, t + u] + (fin[ch][0, t + u] + fin[ch][1, t + u]))
        loop(n_grp, body)

    def step_a(j):
        df = order_of(j)
        side_near(1, df)
        both(0, df, 0)
    loop(4, step_a)
    to_s(2, my_slot)
    to_sibling(2, my_slot)
    line_near(2)
    line_far(2)

    def step_b(j):
        df = order_of(j)
        side_far(1, df)
        both(0, df, 1)
        both(0, df, 3)
    loop(4, step_b)

    def step_c(j):
        df = order_of(j)
        side_near(2, df)
        both(0, df, 2)
    loop(4, step_c)
    to_sel.wait()

    far(0)
    near(0)

    def step_d(j):
        df = order_of(j)
        side_far(2, df)
        both(1, df, 0)
        both(1, df, 1)
        both(1, df, 3)
    loop(4, step_d)

    def step_e(j):
        both(1, order_of(j), 2)
    loop(4, step_e)

    combined(0)
    far(1)
    near(1)
    mine(0)
    finish(0)
    combined(1)
    mine(1)
    finish(1)

    for k in range(1 + CHUNKS):
        bytes_wait(pieces[k].at[0, pl.ds(0, 3)], f_sem.at[k])
        bytes_wait(pieces[k].at[0, pl.ds(0, 12)], s_sem.at[k])
        bytes_wait(pieces[k].at[0], d_sem.at[k])
    bytes_wait(tblb.at[pl.ds(0, 2 * (PLANE - 1))], tsend_sem.at[0])
    bytes_wait(cb.at[pl.ds(0, 3)], csend_sem.at[0])
    for ch in range(CHUNKS):
        bytes_wait(acc[ch].at[pl.ds(0, 3)], rs_send.at[ch])


def tables(pairs, coords, cidx, z):
    n_own = cidx.shape[0]
    pid = jnp.where(pairs[..., 0] >= 0, pairs[..., 0] * 4 + pairs[..., 1], NOPAIR)
    pid = pid.reshape(4, RING, PLANE, 2).transpose(2, 1, 3, 0).reshape(PLANE, 1, 4 * SLOTS)
    pid = jnp.pad(pid, ((0, 0), (0, 0), (0, 128 - 4 * SLOTS)))
    code = jnp.where(coords[:, 0] >= 0, coords[:, 0] * 256 + coords[:, 1], -1)
    code = code.reshape(RING, PLANE, 2).transpose(1, 2, 0)
    code = jnp.broadcast_to(code[..., None], (PLANE, 2, RING, n_own)).reshape(PLANE, 1, 128)
    tbl = jnp.concatenate([pid, code], axis=1).reshape(2 * PLANE, 1, 128)
    own = cidx[:, 0] * 256 + cidx[:, 1]
    at = jnp.arange(RING)[:, None] == z
    crow = jnp.broadcast_to(jnp.where(at, own[None, :], 0)[None], (2, RING, n_own)).reshape(1, 1, 128)
    return tbl, crow


def solution(mesh):
    dev_spec = P(("batch", "k"))

    def per_device(a_loc, b_loc, pair_loc, coord_loc, cidx_loc):
        a, b, cidx = a_loc[0], b_loc[0], cidx_loc[0]
        n_own = cidx.shape[0]
        rows, depth, cols = a.shape[1], a.shape[2], b.shape[2]
        cr = rows // CHUNKS
        tbl, crow = tables(pair_loc[0], coord_loc[0], cidx, lax.axis_index("k") // PLANE)
        f32, i32, bf16 = jnp.float32, jnp.int32, jnp.bfloat16
        dma = pltpu.SemaphoreType.DMA
        out = pl.pallas_call(
            kernel,
            out_shape=jax.ShapeDtypeStruct((n_own, rows, cols), f32),
            in_specs=[pl.BlockSpec(memory_space=pl.ANY)] * 4,
            out_specs=pl.BlockSpec(memory_space=pltpu.VMEM),
            scratch_shapes=[
                pltpu.VMEM((2, LINES, 4, depth, cols), bf16),
                [pltpu.VMEM((2, LINES, 4, cr, depth), bf16) for _ in range(CHUNKS)],
                [pltpu.VMEM((NOPAIR + 1, cr, cols), f32) for _ in range(2)],
                [pltpu.VMEM((NOSLOT + 1, cr, cols), f32) for _ in range(CHUNKS)],
                [pltpu.VMEM((RING, n_own, cr, cols), f32) for _ in range(CHUNKS)],
                [pltpu.VMEM((2, n_own // 2, cr, cols), f32) for _ in range(CHUNKS)],
                [pltpu.VMEM((2, n_own, cr, cols), f32) for _ in range(CHUNKS)],
                pltpu.VMEM((2 * PLANE, 1, 128), i32),
                pltpu.VMEM((RING, 1, 128), i32),
                pltpu.VMEM((PLANE, 128), i32),
                pltpu.SMEM((2 * PLANE, 1, 128), i32),
                pltpu.SMEM((PLANE, 128), i32),
                dma((1 + CHUNKS,)),
                dma((1 + CHUNKS, LINES, 2)), dma((1 + CHUNKS, LINES)),
                dma((1 + CHUNKS,)), dma((1 + CHUNKS,)), dma((1 + CHUNKS,)),
                dma((1,)), dma((1,)), dma((1,)), dma((1,)), dma((2,)), dma((1,)), dma((1,)),
                dma((CHUNKS,)), dma((CHUNKS, 2, n_own // 2 // GROUP)), dma((CHUNKS, 2, n_own // GROUP)),
            ],
            compiler_params=pltpu.CompilerParams(collective_id=0, has_side_effects=True,
                                                 vmem_limit_bytes=60 * 1024 * 1024),
        )(a, b, tbl, crow)
        return out[None]

    return jax.shard_map(per_device, mesh=mesh, in_specs=(dev_spec,) * 5, out_specs=dev_spec, check_vma=False)
```

```python
import jax
import jax.numpy as jnp
from jax import lax
from jax.experimental import pallas as pl
from jax.experimental.pallas import tpu as pltpu
from jax.sharding import PartitionSpec as P

RING = 4
PLANE = 32
LINES = PLANE // 2
SLOTS = 8
NOPAIR = 16
NOSLOT = PLANE * SLOTS
CHUNKS = 2
GROUP = 2
MESH = pl.DeviceIdType.MESH


def order_of(j):
    return j + (j // 2) * (1 - 2 * (j % 2))


def kernel(a_ref, b_ref, pairs_ref, coords_ref, cidx_ref, out_ref, held_b, held_a, held_t, prods, parts, acc, opp, fin,
           cb, tblv, selv, tbl_s, sel_s, local_sem, own_sem, sib_sem, f_sem, s_sem, d_sem, csend_sem, crecv_sem,
           smem_sem, sel_sem, rs_send, opp_sem, fin_sem):
    me = lax.axis_index("k")
    z = me // PLANE
    d = me % PLANE
    y = d // 8
    x = (d // 2) % 4
    c = d % 2
    n_own = out_ref.shape[0]
    half_own = n_own // 2
    n_grp = half_own // GROUP
    chunk_rows = out_ref.shape[1] // CHUNKS
    cols = out_ref.shape[2]

    def dev(zz, yy, xx, cc):
        return {"k": ((zz * 4 + yy) * 4 + xx) * 2 + cc}

    sibling = dev(z, y, x, 1 - c)

    def f_dev(off):
        return dev(z, (y + off * c) % 4, (x + off * (1 - c)) % 4, c)

    def s_dev(off):
        return dev(z, (y + off * (1 - c)) % 4, (x + off * c) % 4, c)

    def z_dev(off):
        return {"k": ((z + off) % 4) * PLANE + d}

    def slot_of(core, df, ds):
        sx = (x + df * (1 - core) + ds * core) % 4
        sy = (y + df * core + ds * (1 - core)) % 4
        return sy * 4 + sx

    barrier = pltpu.get_barrier_semaphore()

    for peer in (f_dev(1), f_dev(3), s_dev(1), s_dev(3), sibling, z_dev(1), z_dev(3)):
        pl.semaphore_signal(barrier, inc=1, device_id=peer, device_id_type=MESH)

    my_slot = y * 4 + x
    z_up, z_two, z_down = (z + 1) % 4, (z + 2) % 4, (z + 3) % 4
    pieces = [held_b] + list(held_a) + [held_t]
    tab = 1 + CHUNKS

    loads = [pltpu.make_async_copy(b_ref, held_b.at[c, my_slot], local_sem.at[0])]
    for ch in range(CHUNKS):
        loads.append(pltpu.make_async_copy(a_ref.at[:, pl.ds(ch * chunk_rows, chunk_rows)], held_a[ch].at[c, my_slot],
                                           local_sem.at[1 + ch]))
    for cp in loads:
        cp.start()
    zero = jnp.zeros((chunk_rows, cols), jnp.float32)
    for ref in prods:
        ref[NOPAIR] = zero
    for ref in parts:
        ref[NOSLOT] = zero

    def block_code(ij):
        return jnp.where(ij[0:1] >= 0, ij[0:1] * 256 + ij[1:2], -1)

    code = block_code(coords_ref[...])
    for h in (0, 1):
        span = pl.ds(128 * h, 128)
        for u in range(4):
            left = pairs_ref[u, 0:1, span]
            held_t[c, my_slot, h, u:u + 1] = jnp.where(left >= 0, left * 4 + pairs_ref[u, 1:2, span], NOPAIR)
        held_t[c, my_slot, h, 4:5] = code[:, 128 * h:128 * h + 128]
        held_t[c, my_slot, h, 5:8] = jnp.zeros((3, 128), jnp.int32)
    cb[z] = jnp.full((8, 128), -2, jnp.int32)
    cb[z, 0:1, 0:n_own] = block_code(cidx_ref[...])

    pl.semaphore_wait(barrier, 7)

    def whole(k, core, slot):
        return pieces[k].at[core, slot]

    def half(k, core, slot, h):
        n_half = pieces[k].shape[2] // 2
        return pieces[k].at[core, slot, pl.ds(n_half * h, n_half)]

    def send(ref, target, send_sem, recv_sem):
        pltpu.make_async_remote_copy(src_ref=ref, dst_ref=ref, send_sem=send_sem, recv_sem=recv_sem,
                                     device_id=target, device_id_type=MESH).start()

    def bytes_wait(ref, sem):
        pltpu.make_async_copy(ref, ref, sem).wait()

    def to_sibling(k, slot):
        send(whole(k, c, slot), sibling, d_sem.at[k], sib_sem.at[k, slot])

    def to_f(k, slot):
        for off in (1, 3):
            send(whole(k, c, slot), f_dev(off), f_sem.at[k], own_sem.at[k, slot, 0])

    def to_s(k, slot):
        for off in (1, 3):
            send(whole(k, c, slot), s_dev(off), s_sem.at[k], own_sem.at[k, slot, 0])

    def got_whole(k, slot):
        bytes_wait(whole(k, c, slot), own_sem.at[k, slot, 0])

    def got_halves(k, slot):
        for h in (0, 1):
            bytes_wait(half(k, c, slot, h), own_sem.at[k, slot, h])

    def line_near(k):
        for df, h, off in ((1, 1, 3), (3, 0, 1)):
            slot = slot_of(c, df, 0)
            got_whole(k, slot)
            send(half(k, c, slot, h), f_dev(off), f_sem.at[k], own_sem.at[k, slot, h])
            to_s(k, slot)
            to_sibling(k, slot)

    def line_far(k):
        slot = slot_of(c, 2, 0)
        got_halves(k, slot)
        to_s(k, slot)
        to_sibling(k, slot)

    def side_near(k, df):
        for ds, h, off in ((1, 1, 3), (3, 0, 1)):
            slot = slot_of(c, df, ds)
            got_whole(k, slot)
            send(half(k, c, slot, h), s_dev(off), s_sem.at[k], own_sem.at[k, slot, h])
            to_sibling(k, slot)

    def side_far(k, df):
        slot = slot_of(c, df, 2)
        got_halves(k, slot)
        to_sibling(k, slot)

    loads[0].wait()
    to_f(0, my_slot)
    to_s(0, my_slot)
    to_sibling(0, my_slot)
    to_f(tab, my_slot)
    to_s(tab, my_slot)
    to_sibling(tab, my_slot)

    def push_codes(row, off):
        pltpu.make_async_remote_copy(
            src_ref=cb.at[row], dst_ref=cb.at[row], send_sem=csend_sem.at[0], recv_sem=crecv_sem.at[row],
            device_id=z_dev(off), device_id_type=MESH).start()

    push_codes(z, 1)
    push_codes(z, 3)
    loads[1].wait()
    to_f(1, my_slot)
    to_s(1, my_slot)
    to_sibling(1, my_slot)
    loads[2].wait()

    line_near(0)
    line_near(tab)
    side_near(0, 0)
    side_near(tab, 0)
    line_near(1)
    side_near(1, 0)
    line_far(tab)
    line_far(0)
    line_far(1)
    bytes_wait(cb.at[z_down], crecv_sem.at[z_down])
    push_codes(z_down, 1)
    side_near(tab, 1)
    side_near(0, 1)
    side_near(tab, 3)
    side_near(tab, 2)
    side_near(0, 3)
    for j in range(4):
        side_far(tab, order_of(j))
    side_far(0, 0)

    lane = lax.broadcasted_iota(jnp.int32, (8, 128), 1)
    shift = 2 * PLANE * 2 - 2 * d

    def pick(slot, tables):
        picked = []
        for core, table in enumerate(tables):
            for h in (0, 1):
                moved = pltpu.roll(held_t[core, slot, h], (shift + 4 * slot + 2 * h) % 128, 1)
                table = jnp.where((lane % 64) // 2 == 2 * slot + h, moved, table)
            picked.append(table)
        return tuple(picked)

    def sib_tables(slot, carry):
        bytes_wait(whole(tab, 1 - c, slot), sib_sem.at[tab, slot])
        return carry

    lax.fori_loop(0, LINES, sib_tables, 0)
    none = jnp.zeros((8, 128), jnp.int32)
    picked = lax.fori_loop(0, LINES, pick, (none, none))
    for core in (0, 1):
        tblv[core] = picked[core]

    sub = lax.broadcasted_iota(jnp.int32, (n_own, 128), 0)
    lane = lax.broadcasted_iota(jnp.int32, (n_own, 128), 1)
    for row in (z_up, z_two):
        bytes_wait(cb.at[row], crecv_sem.at[row])
    wanted = jnp.zeros((n_own, 128), jnp.int32)
    for zz in range(RING):
        column = jnp.where(sub == lane, jnp.broadcast_to(cb[zz, 0:1], (n_own, 128)), 0)
        for bit in range(7):
            column = column + pltpu.roll(column, 1 << bit, 1)
        wanted = jnp.where(2 * (lane // 2 % 2) + lane // 64 == zz, column, wanted)
    for core in (0, 1):
        source = (lane % 64 // 4) * 2 + core
        index = source * SLOTS + 2 * (2 * (lane // 2 % 2) + lane // 64) + lane % 2
        hit = jnp.where(jnp.broadcast_to(picked[core][4:5], (n_own, 128)) == wanted, index - NOSLOT, 0)
        selv[core] = NOSLOT + jnp.where(hit != 0, hit, pltpu.roll(hit, 127, 1))
    to_smem = pltpu.make_async_copy(tblv, tbl_s, smem_sem.at[0])
    to_sel = pltpu.make_async_copy(selv, sel_s, sel_sem.at[0])
    to_smem.start()
    to_sel.start()
    to_smem.wait()
    to_sel.wait()

    def compute(ch, core, df, ds, prod):
        slot = slot_of(core, df, ds)
        lhs = held_a[ch][core, slot].reshape(4 * chunk_rows, -1)
        for pair in (0, 1):
            rhs = jnp.concatenate([held_b[core, slot, 2 * pair], held_b[core, slot, 2 * pair + 1]], axis=1)
            res = jnp.dot(lhs, rhs, preferred_element_type=jnp.float32)
            for a in range(4):
                for b in (0, 1):
                    prod[a * 4 + 2 * pair + b] = res[a * chunk_rows:(a + 1) * chunk_rows, b * cols:(b + 1) * cols]
        src = slot * 2 + core
        for j in range(SLOTS):
            at_lane = 64 * (j // 2 % 2) + 4 * slot + 2 * (j // 4) + j % 2
            total = prod[tbl_s[core, 0, at_lane]]
            for u in (1, 2, 3):
                total = total + prod[tbl_s[core, u, at_lane]]
            parts[ch][src * SLOTS + j] = total.astype(jnp.bfloat16).astype(jnp.float32)

    def both(ch, df, ds, first=True):
        slot = slot_of(1 - c, df, ds)
        if ch == 0:
            bytes_wait(whole(0, 1 - c, slot), sib_sem.at[0, slot])
        bytes_wait(whole(1 + ch, 1 - c, slot), sib_sem.at[1 + ch, slot])
        compute(ch, c, df, ds, prods[0])
        compute(ch, 1 - c, df, ds, prods[1])

    def loop(n, body):
        def run(j, carry):
            body(j)
            return carry
        lax.fori_loop(0, n, run, 0)

    def block_sum(ch, zz, t):
        base = 64 * (zz % 2) + 2 * (zz // 2)

        def add(p8, total):
            for u in range(8):
                total = total + parts[ch][sel_s[u % 2, t, base + 4 * (p8 * 4 + u // 2)]]
            return total
        return lax.fori_loop(0, PLANE // 8, add, zero)

    def z_push(ch, zz, t, dst, recv, off):
        pltpu.make_async_remote_copy(
            src_ref=acc[ch].at[zz, pl.ds(t, GROUP)], dst_ref=dst, send_sem=rs_send.at[ch], recv_sem=recv,
            device_id=z_dev(off), device_id_type=MESH).start()

    def far(ch):
        def body(g):
            t = g * GROUP
            for u in range(GROUP):
                acc[ch][z_two, t + u] = block_sum(ch, z_two, t + u)
                acc[ch][z_two, t + half_own + u] = block_sum(ch, z_two, t + half_own + u)
            z_push(ch, z_two, t, opp[ch].at[0, pl.ds(t, GROUP)], opp_sem.at[ch, 0, g], 1)
            z_push(ch, z_two, t + half_own, opp[ch].at[1, pl.ds(t, GROUP)], opp_sem.at[ch, 1, g], 3)
        loop(n_grp, body)

    def near(ch):
        def body(g):
            t = g * GROUP
            for u in range(GROUP):
                acc[ch][z_up, t + half_own + u] = block_sum(ch, z_up, t + half_own + u)
                acc[ch][z_down, t + u] = block_sum(ch, z_down, t + u)
            z_push(ch, z_up, t + half_own, fin[ch].at[0, pl.ds(t + half_own, GROUP)], fin_sem.at[ch, 0, g + n_grp], 1)
            z_push(ch, z_down, t, fin[ch].at[1, pl.ds(t, GROUP)], fin_sem.at[ch, 1, g], 3)
        loop(n_grp, body)

    def combined(ch):
        def body(g):
            t = g * GROUP
            up = [block_sum(ch, z_up, t + u) for u in range(GROUP)]
            for u in range(GROUP):
                acc[ch][z_up, t + u] = up[u]
            down = [block_sum(ch, z_down, t + half_own + u) for u in range(GROUP)]
            for u in range(GROUP):
                acc[ch][z_down, t + half_own + u] = down[u]
            bytes_wait(opp[ch].at[0, pl.ds(t, GROUP)], opp_sem.at[ch, 0, g])
            bytes_wait(opp[ch].at[1, pl.ds(t, GROUP)], opp_sem.at[ch, 1, g])
            for u in range(GROUP):
                acc[ch][z_up, t + u] += opp[ch][0, t + u]
                acc[ch][z_down, t + half_own + u] += opp[ch][1, t + u]
            z_push(ch, z_up, t, fin[ch].at[0, pl.ds(t, GROUP)], fin_sem.at[ch, 0, g], 1)
            z_push(ch, z_down, t + half_own, fin[ch].at[1, pl.ds(t + half_own, GROUP)], fin_sem.at[ch, 1, g + n_grp], 3)
        loop(n_grp, body)

    def mine(ch):
        def body(t):
            acc[ch][z, t] = block_sum(ch, z, t)
        loop(n_own, body)

    def finish(ch):
        def body(g):
            for gg in (g, g + n_grp):
                t = gg * GROUP
                for side in (0, 1):
                    bytes_wait(fin[ch].at[side, pl.ds(t, GROUP)], fin_sem.at[ch, side, gg])
                for u in range(GROUP):
                    out_ref[t + u, pl.ds(ch * chunk_rows, chunk_rows)] = (
                        acc[ch][z, t + u] + (fin[ch][0, t + u] + fin[ch][1, t + u]))
        loop(n_grp, body)

    def at(n, step, *events):
        @pl.when(n == step)
        def _():
            for event in events:
                event()

    def step_a(n):
        at(n, 0, lambda: side_near(1, 1))
        at(n, 1, lambda: side_near(1, 3))
        at(n, 2, lambda: side_far(1, 0), lambda: to_f(2, my_slot), lambda: to_s(2, my_slot),
           lambda: to_sibling(2, my_slot))
        at(n, 5, lambda: side_near(0, 2))
        at(n, 7, lambda: side_near(1, 2))
        at(n, 9, lambda: side_far(0, 1))
        at(n, 11, lambda: side_far(0, 3))
        m = n % 3
        both(0, order_of(n // 3), m + m // 2)
    loop(12, step_a)

    def step_b(j):
        at(j, 0, lambda: line_near(2))
        at(j, 1, lambda: side_far(1, 1))
        at(j, 2, lambda: side_far(1, 3))
        at(j, 3, lambda: side_far(0, 2), lambda: side_far(1, 2))
        both(0, order_of(j), 2)
    loop(4, step_b)
    side_near(2, 0)
    line_far(2)

    far(0)
    near(0)

    def step_c(n):
        at(n, 0, lambda: side_near(2, 1))
        at(n, 1, lambda: side_near(2, 3))
        at(n, 2, lambda: side_far(2, 0))
        at(n, 3, lambda: side_near(2, 2))
        at(n, 5, lambda: side_far(2, 1))
        at(n, 6, lambda: side_far(2, 3))
        at(n, 8, lambda: side_far(2, 2))
        m = n % 3
        both(1, order_of(n // 3), m + m // 2)
    loop(12, step_c)

    def step_d(j):
        both(1, order_of(j), 2)
    loop(4, step_d)

    combined(0)
    far(1)
    near(1)
    mine(0)
    finish(0)
    combined(1)
    mine(1)
    finish(1)

    for k in range(2 + CHUNKS):
        bytes_wait(pieces[k].at[0, pl.ds(0, 3)], f_sem.at[k])
        bytes_wait(pieces[k].at[0, pl.ds(0, 12)], s_sem.at[k])
        bytes_wait(pieces[k].at[0], d_sem.at[k])
    bytes_wait(cb.at[pl.ds(0, 3)], csend_sem.at[0])
    for ch in range(CHUNKS):
        bytes_wait(acc[ch].at[pl.ds(0, 3)], rs_send.at[ch])


def solution(mesh):
    dev_spec = P(("batch", "k"))

    def per_device(a_loc, b_loc, pair_loc, coord_loc, cidx_loc):
        a, b = a_loc[0], b_loc[0]
        pairs, coords, cidx = (jnp.swapaxes(v[0], -1, -2) for v in (pair_loc, coord_loc, cidx_loc))
        n_own = cidx.shape[1]
        rows, depth, cols = a.shape[1], a.shape[2], b.shape[2]
        cr = rows // CHUNKS
        f32, i32, bf16 = jnp.float32, jnp.int32, jnp.bfloat16
        dma = pltpu.SemaphoreType.DMA
        out = pl.pallas_call(
            kernel,
            out_shape=jax.ShapeDtypeStruct((n_own, rows, cols), f32),
            in_specs=[pl.BlockSpec(memory_space=pl.ANY)] * 2 + [pl.BlockSpec(memory_space=pltpu.VMEM)] * 3,
            out_specs=pl.BlockSpec(memory_space=pltpu.VMEM),
            scratch_shapes=[
                pltpu.VMEM((2, LINES, 4, depth, cols), bf16),
                [pltpu.VMEM((2, LINES, 4, cr, depth), bf16) for _ in range(CHUNKS)],
                pltpu.VMEM((2, LINES, 2, 8, 128), i32),
                [pltpu.VMEM((NOPAIR + 1, cr, cols), f32) for _ in range(2)],
                [pltpu.VMEM((NOSLOT + 1, cr, cols), f32) for _ in range(CHUNKS)],
                [pltpu.VMEM((RING, n_own, cr, cols), f32) for _ in range(CHUNKS)],
                [pltpu.VMEM((2, n_own // 2, cr, cols), f32) for _ in range(CHUNKS)],
                [pltpu.VMEM((2, n_own, cr, cols), f32) for _ in range(CHUNKS)],
                pltpu.VMEM((RING, 8, 128), i32),
                pltpu.VMEM((2, 8, 128), i32),
                pltpu.VMEM((2, n_own, 128), i32),
                pltpu.SMEM((2, 8, 128), i32),
                pltpu.SMEM((2, n_own, 128), i32),
                dma((1 + CHUNKS,)),
                dma((2 + CHUNKS, LINES, 2)), dma((2 + CHUNKS, LINES)),
                dma((2 + CHUNKS,)), dma((2 + CHUNKS,)), dma((2 + CHUNKS,)),
                dma((1,)), dma((RING,)), dma((1,)), dma((1,)),
                dma((CHUNKS,)), dma((CHUNKS, 2, n_own // 2 // GROUP)), dma((CHUNKS, 2, n_own // GROUP)),
            ],
            compiler_params=pltpu.CompilerParams(collective_id=0, has_side_effects=True,
                                                 vmem_limit_bytes=60 * 1024 * 1024),
        )(a, b, pairs, coords, cidx)
        return out[None]

    return jax.shard_map(per_device, mesh=mesh, in_specs=(dev_spec,) * 5, out_specs=dev_spec, check_vma=False)
```

```python
import jax
import jax.numpy as jnp
from jax import lax
from jax.experimental import pallas as pl
from jax.experimental.pallas import tpu as pltpu
from jax.sharding import PartitionSpec as P

RING = 4
PLANE = 32
LINES = PLANE // 2
SLOTS = 8
NOPAIR = 16
NOSLOT = PLANE * SLOTS
CHUNKS = 2
GROUP = 2
MESH = pl.DeviceIdType.MESH


def order_of(j):
    return j + (j // 2) * (1 - 2 * (j % 2))


def kernel(a_ref, b_ref, pairs_hbm, coords_hbm, cidx_hbm, out_ref, pairs_ref, coords_ref, cidx_ref, result, held_b, held_a, held_t, prods, parts, acc, opp, fin,
           cb, tblv, selv, tbl_s, sel_s, ints_sem, out_sem, local_sem, own_sem, sib_sem, f_sem, s_sem, d_sem, csend_sem, crecv_sem,
           smem_sem, sel_sem, rs_send, opp_sem, fin_sem):
    me = lax.axis_index("k")
    z = me // PLANE
    d = me % PLANE
    y = d // 8
    x = (d // 2) % 4
    c = d % 2
    n_own = out_ref.shape[0]
    half_own = n_own // 2
    n_grp = half_own // GROUP
    chunk_rows = out_ref.shape[1] // CHUNKS
    cols = out_ref.shape[2]

    def dev(zz, yy, xx, cc):
        return {"k": ((zz * 4 + yy) * 4 + xx) * 2 + cc}

    sibling = dev(z, y, x, 1 - c)

    def f_dev(off):
        return dev(z, (y + off * c) % 4, (x + off * (1 - c)) % 4, c)

    def s_dev(off):
        return dev(z, (y + off * (1 - c)) % 4, (x + off * c) % 4, c)

    def z_dev(off):
        return {"k": ((z + off) % 4) * PLANE + d}

    def slot_of(core, df, ds):
        sx = (x + df * (1 - core) + ds * core) % 4
        sy = (y + df * core + ds * (1 - core)) % 4
        return sy * 4 + sx

    barrier = pltpu.get_barrier_semaphore()

    for peer in [sibling] + [dev_of(off) for dev_of in (f_dev, s_dev, z_dev) for off in (2, 1, 3)]:
        pl.semaphore_signal(barrier, inc=1, device_id=peer, device_id_type=MESH)

    my_slot = y * 4 + x
    z_up, z_two, z_down = (z + 1) % 4, (z + 2) % 4, (z + 3) % 4
    pieces = [held_b] + list(held_a) + [held_t]
    tab = 1 + CHUNKS

    ints = [pltpu.make_async_copy(src, dst, ints_sem.at[i]) for i, (src, dst) in enumerate(
        ((pairs_hbm, pairs_ref), (coords_hbm, coords_ref), (cidx_hbm, cidx_ref)))]
    loads = [pltpu.make_async_copy(b_ref, held_b.at[c, my_slot], local_sem.at[0])]
    for ch in range(CHUNKS):
        loads.append(pltpu.make_async_copy(a_ref.at[:, pl.ds(ch * chunk_rows, chunk_rows)], held_a[ch].at[c, my_slot],
                                           local_sem.at[1 + ch]))
    for cp in ints + loads:
        cp.start()
    zero = jnp.zeros((chunk_rows, cols), jnp.float32)
    for ref in prods:
        ref[NOPAIR] = zero
    for ref in parts:
        ref[NOSLOT] = zero

    for cp in ints:
        cp.wait()
    def block_code(ij):
        return jnp.where(ij[0:1] >= 0, ij[0:1] * 256 + ij[1:2], -1)

    code = block_code(coords_ref[...])
    for h in (0, 1):
        span = pl.ds(128 * h, 128)
        for u in range(4):
            left = pairs_ref[u, 0:1, span]
            held_t[c, my_slot, h, u:u + 1] = jnp.where(left >= 0, left * 4 + pairs_ref[u, 1:2, span], NOPAIR)
        held_t[c, my_slot, h, 4:5] = code[:, 128 * h:128 * h + 128]
        held_t[c, my_slot, h, 5:8] = jnp.zeros((3, 128), jnp.int32)
    cb[z] = jnp.full((8, 128), -2, jnp.int32)
    cb[z, 0:1, 0:n_own] = block_code(cidx_ref[...])

    pl.semaphore_wait(barrier, 10)

    def whole(k, core, slot):
        return pieces[k].at[core, slot]

    def half(k, core, slot, h):
        n_half = pieces[k].shape[2] // 2
        return pieces[k].at[core, slot, pl.ds(n_half * h, n_half)]

    def send(ref, target, send_sem, recv_sem):
        pltpu.make_async_remote_copy(src_ref=ref, dst_ref=ref, send_sem=send_sem, recv_sem=recv_sem,
                                     device_id=target, device_id_type=MESH).start()

    def bytes_wait(ref, sem):
        pltpu.make_async_copy(ref, ref, sem).wait()

    def to_sibling(k, slot):
        send(whole(k, c, slot), sibling, d_sem.at[k], sib_sem.at[k, slot])

    def to_f(k, slot):
        for off in (1, 3):
            send(whole(k, c, slot), f_dev(off), f_sem.at[k], own_sem.at[k, slot, 0])

    def to_s(k, slot):
        for off in (1, 3):
            send(whole(k, c, slot), s_dev(off), s_sem.at[k], own_sem.at[k, slot, 0])

    def got_whole(k, slot):
        bytes_wait(whole(k, c, slot), own_sem.at[k, slot, 0])

    def got_halves(k, slot):
        for h in (0, 1):
            bytes_wait(half(k, c, slot, h), own_sem.at[k, slot, h])

    def line_near(k):
        for df, h, off in ((1, 1, 3), (3, 0, 1)):
            slot = slot_of(c, df, 0)
            got_whole(k, slot)
            send(half(k, c, slot, h), f_dev(off), f_sem.at[k], own_sem.at[k, slot, h])
            to_s(k, slot)
            to_sibling(k, slot)

    def line_far(k):
        slot = slot_of(c, 2, 0)
        got_halves(k, slot)
        to_s(k, slot)
        to_sibling(k, slot)

    def side_near(k, df):
        for ds, h, off in ((1, 1, 3), (3, 0, 1)):
            slot = slot_of(c, df, ds)
            got_whole(k, slot)
            send(half(k, c, slot, h), s_dev(off), s_sem.at[k], own_sem.at[k, slot, h])
            to_sibling(k, slot)

    def side_far(k, df):
        slot = slot_of(c, df, 2)
        got_halves(k, slot)
        to_sibling(k, slot)

    def t_line(slot):
        for off in (2, 1, 3):
            send(whole(tab, c, slot), s_dev(off), s_sem.at[tab], own_sem.at[tab, slot, 0])
        to_sibling(tab, slot)

    for off in (2, 1, 3):
        send(whole(tab, c, my_slot), f_dev(off), f_sem.at[tab], own_sem.at[tab, my_slot, 0])
    t_line(my_slot)
    for off in (2, 1, 3):
        pltpu.make_async_remote_copy(
            src_ref=cb.at[z], dst_ref=cb.at[z], send_sem=csend_sem.at[0], recv_sem=crecv_sem.at[z],
            device_id=z_dev(off), device_id_type=MESH).start()
    for k in (0, 1):
        loads[k].wait()
        to_f(k, my_slot)
        to_s(k, my_slot)
        to_sibling(k, my_slot)
    loads[2].wait()

    for df in (1, 3, 2):
        slot = slot_of(c, df, 0)
        got_whole(tab, slot)
        t_line(slot)
    line_near(0)
    side_near(0, 0)
    line_near(1)
    side_near(1, 0)

    def t_side(n, carry):
        slot = slot_of(c, n // 3, 1 + n % 3)
        got_whole(tab, slot)
        to_sibling(tab, slot)
        return carry

    lax.fori_loop(0, 12, t_side, 0)
    line_far(0)
    line_far(1)
    side_near(0, 1)

    lane = lax.broadcasted_iota(jnp.int32, (8, 128), 1)
    shift = 2 * PLANE * 2 - 2 * d

    def pick(slot, tables):
        picked = []
        for core, table in enumerate(tables):
            for h in (0, 1):
                moved = pltpu.roll(held_t[core, slot, h], (shift + 4 * slot + 2 * h) % 128, 1)
                table = jnp.where((lane % 64) // 2 == 2 * slot + h, moved, table)
            picked.append(table)
        return tuple(picked)

    def sib_tables(slot, carry):
        bytes_wait(whole(tab, 1 - c, slot), sib_sem.at[tab, slot])
        return carry

    lax.fori_loop(0, LINES, sib_tables, 0)
    none = jnp.zeros((8, 128), jnp.int32)
    picked = lax.fori_loop(0, LINES, pick, (none, none))
    for core in (0, 1):
        tblv[core] = picked[core]

    sub = lax.broadcasted_iota(jnp.int32, (n_own, 128), 0)
    lane = lax.broadcasted_iota(jnp.int32, (n_own, 128), 1)
    for row in (z_up, z_two, z_down):
        bytes_wait(cb.at[row], crecv_sem.at[row])
    wanted = jnp.zeros((n_own, 128), jnp.int32)
    for zz in range(RING):
        column = jnp.where(sub == lane, jnp.broadcast_to(cb[zz, 0:1], (n_own, 128)), 0)
        for bit in range(7):
            column = column + pltpu.roll(column, 1 << bit, 1)
        wanted = jnp.where(2 * (lane // 2 % 2) + lane // 64 == zz, column, wanted)
    for core in (0, 1):
        source = (lane % 64 // 4) * 2 + core
        index = source * SLOTS + 2 * (2 * (lane // 2 % 2) + lane // 64) + lane % 2
        hit = jnp.where(jnp.broadcast_to(picked[core][4:5], (n_own, 128)) == wanted, index - NOSLOT, 0)
        selv[core] = NOSLOT + jnp.where(hit != 0, hit, pltpu.roll(hit, 127, 1))
    to_smem = pltpu.make_async_copy(tblv, tbl_s, smem_sem.at[0])
    to_sel = pltpu.make_async_copy(selv, sel_s, sel_sem.at[0])
    to_smem.start()
    to_sel.start()
    side_near(0, 3)
    side_far(0, 0)
    to_smem.wait()
    to_sel.wait()

    def compute(ch, core, df, ds, prod):
        slot = slot_of(core, df, ds)
        lhs = held_a[ch][core, slot].reshape(4 * chunk_rows, -1)
        for pair in (0, 1):
            rhs = jnp.concatenate([held_b[core, slot, 2 * pair], held_b[core, slot, 2 * pair + 1]], axis=1)
            res = jnp.dot(lhs, rhs, preferred_element_type=jnp.float32)
            for a in range(4):
                for b in (0, 1):
                    prod[a * 4 + 2 * pair + b] = res[a * chunk_rows:(a + 1) * chunk_rows, b * cols:(b + 1) * cols]
        src = slot * 2 + core
        for j in range(SLOTS):
            at_lane = 64 * (j // 2 % 2) + 4 * slot + 2 * (j // 4) + j % 2
            total = prod[tbl_s[core, 0, at_lane]]
            for u in (1, 2, 3):
                total = total + prod[tbl_s[core, u, at_lane]]
            parts[ch][src * SLOTS + j] = total.astype(jnp.bfloat16).astype(jnp.float32)

    def both(ch, df, ds, first=True):
        slot = slot_of(1 - c, df, ds)
        if ch == 0:
            bytes_wait(whole(0, 1 - c, slot), sib_sem.at[0, slot])
        bytes_wait(whole(1 + ch, 1 - c, slot), sib_sem.at[1 + ch, slot])
        compute(ch, c, df, ds, prods[0])
        compute(ch, 1 - c, df, ds, prods[1])

    def loop(n, body):
        def run(j, carry):
            body(j)
            return carry
        lax.fori_loop(0, n, run, 0)

    def block_sum(ch, zz, t):
        base = 64 * (zz % 2) + 2 * (zz // 2)

        def add(p8, total):
            for u in range(8):
                total = total + parts[ch][sel_s[u % 2, t, base + 4 * (p8 * 4 + u // 2)]]
            return total
        return lax.fori_loop(0, PLANE // 8, add, zero)

    def z_push(ch, zz, t, dst, recv, off):
        pltpu.make_async_remote_copy(
            src_ref=acc[ch].at[zz, pl.ds(t, GROUP)], dst_ref=dst, send_sem=rs_send.at[ch], recv_sem=recv,
            device_id=z_dev(off), device_id_type=MESH).start()

    def far(ch):
        def body(g):
            t = g * GROUP
            for u in range(GROUP):
                acc[ch][z_two, t + u] = block_sum(ch, z_two, t + u)
                acc[ch][z_two, t + half_own + u] = block_sum(ch, z_two, t + half_own + u)
            z_push(ch, z_two, t, opp[ch].at[0, pl.ds(t, GROUP)], opp_sem.at[ch, 0, g], 1)
            z_push(ch, z_two, t + half_own, opp[ch].at[1, pl.ds(t, GROUP)], opp_sem.at[ch, 1, g], 3)
        loop(n_grp, body)

    def near(ch):
        def body(g):
            t = g * GROUP
            for u in range(GROUP):
                acc[ch][z_up, t + half_own + u] = block_sum(ch, z_up, t + half_own + u)
                acc[ch][z_down, t + u] = block_sum(ch, z_down, t + u)
            z_push(ch, z_up, t + half_own, fin[ch].at[0, pl.ds(t + half_own, GROUP)], fin_sem.at[ch, 0, g + n_grp], 1)
            z_push(ch, z_down, t, fin[ch].at[1, pl.ds(t, GROUP)], fin_sem.at[ch, 1, g], 3)
        loop(n_grp, body)

    def combined(ch):
        def body(g):
            t = g * GROUP
            up = [block_sum(ch, z_up, t + u) for u in range(GROUP)]
            for u in range(GROUP):
                acc[ch][z_up, t + u] = up[u]
            down = [block_sum(ch, z_down, t + half_own + u) for u in range(GROUP)]
            for u in range(GROUP):
                acc[ch][z_down, t + half_own + u] = down[u]
            bytes_wait(opp[ch].at[0, pl.ds(t, GROUP)], opp_sem.at[ch, 0, g])
            bytes_wait(opp[ch].at[1, pl.ds(t, GROUP)], opp_sem.at[ch, 1, g])
            for u in range(GROUP):
                acc[ch][z_up, t + u] += opp[ch][0, t + u]
                acc[ch][z_down, t + half_own + u] += opp[ch][1, t + u]
            z_push(ch, z_up, t, fin[ch].at[0, pl.ds(t, GROUP)], fin_sem.at[ch, 0, g], 1)
            z_push(ch, z_down, t + half_own, fin[ch].at[1, pl.ds(t + half_own, GROUP)], fin_sem.at[ch, 1, g + n_grp], 3)
        loop(n_grp, body)

    def mine(ch):
        def body(t):
            acc[ch][z, t] = block_sum(ch, z, t)
        loop(n_own, body)

    def out_copy(gg):
        span = pl.ds(gg * GROUP, GROUP)
        return pltpu.make_async_copy(result.at[span], out_ref.at[span], out_sem.at[gg])

    def finish(ch):
        def body(g):
            for gg in (g, g + n_grp):
                t = gg * GROUP
                for side in (0, 1):
                    bytes_wait(fin[ch].at[side, pl.ds(t, GROUP)], fin_sem.at[ch, side, gg])
                for u in range(GROUP):
                    result[t + u, pl.ds(ch * chunk_rows, chunk_rows)] = (
                        acc[ch][z, t + u] + (fin[ch][0, t + u] + fin[ch][1, t + u]))
                if ch == CHUNKS - 1:
                    out_copy(gg).start()
        loop(n_grp, body)

    def at(n, step, *events):
        @pl.when(n == step)
        def _():
            for event in events:
                event()

    def step_a(n):
        at(n, 0, lambda: side_near(1, 1))
        at(n, 1, lambda: side_near(1, 3))
        at(n, 2, lambda: side_far(1, 0), lambda: to_f(2, my_slot), lambda: to_s(2, my_slot),
           lambda: to_sibling(2, my_slot))
        at(n, 5, lambda: side_near(0, 2))
        at(n, 7, lambda: side_near(1, 2))
        at(n, 9, lambda: side_far(0, 1))
        at(n, 11, lambda: side_far(0, 3))
        m = n % 3
        both(0, order_of(n // 3), m + m // 2)
    loop(12, step_a)

    def step_b(j):
        at(j, 0, lambda: line_near(2))
        at(j, 1, lambda: side_far(1, 1))
        at(j, 2, lambda: side_far(1, 3))
        at(j, 3, lambda: side_far(0, 2), lambda: side_far(1, 2))
        both(0, order_of(j), 2)
    loop(4, step_b)
    side_near(2, 0)
    line_far(2)

    far(0)
    near(0)

    def step_c(n):
        at(n, 0, lambda: side_near(2, 1))
        at(n, 1, lambda: side_near(2, 3))
        at(n, 2, lambda: side_far(2, 0))
        at(n, 3, lambda: side_near(2, 2))
        at(n, 5, lambda: side_far(2, 1))
        at(n, 6, lambda: side_far(2, 3))
        at(n, 8, lambda: side_far(2, 2))
        m = n % 3
        both(1, order_of(n // 3), m + m // 2)
    loop(12, step_c)

    def step_d(j):
        both(1, order_of(j), 2)
    loop(4, step_d)

    combined(0)
    far(1)
    near(1)
    mine(0)
    finish(0)
    combined(1)
    mine(1)
    finish(1)

    loop(2 * n_grp, lambda gg: out_copy(gg).wait())
    bytes_wait(held_t.at[0, pl.ds(0, 3)], f_sem.at[tab])
    bytes_wait(held_t.at[0, pl.ds(0, 12)], s_sem.at[tab])
    bytes_wait(held_t.at[0], d_sem.at[tab])
    for k in range(1 + CHUNKS):
        bytes_wait(pieces[k].at[0, pl.ds(0, 3)], f_sem.at[k])
        bytes_wait(pieces[k].at[0, pl.ds(0, 12)], s_sem.at[k])
        bytes_wait(pieces[k].at[0], d_sem.at[k])
    bytes_wait(cb.at[pl.ds(0, 3)], csend_sem.at[0])
    for ch in range(CHUNKS):
        bytes_wait(acc[ch].at[pl.ds(0, 3)], rs_send.at[ch])


def solution(mesh):
    dev_spec = P(("batch", "k"))

    def per_device(a_loc, b_loc, pair_loc, coord_loc, cidx_loc):
        a, b = a_loc[0], b_loc[0]
        pairs, coords, cidx = (jnp.swapaxes(v[0], -1, -2) for v in (pair_loc, coord_loc, cidx_loc))
        n_own = cidx.shape[1]
        rows, depth, cols = a.shape[1], a.shape[2], b.shape[2]
        cr = rows // CHUNKS
        f32, i32, bf16 = jnp.float32, jnp.int32, jnp.bfloat16
        dma = pltpu.SemaphoreType.DMA
        out = pl.pallas_call(
            kernel,
            out_shape=jax.ShapeDtypeStruct((n_own, rows, cols), f32),
            in_specs=[pl.BlockSpec(memory_space=pl.ANY)] * 5,
            out_specs=pl.BlockSpec(memory_space=pl.ANY),
            scratch_shapes=[
                pltpu.VMEM(pairs.shape, i32), pltpu.VMEM(coords.shape, i32), pltpu.VMEM(cidx.shape, i32),
                pltpu.VMEM((n_own, rows, cols), f32),
                pltpu.VMEM((2, LINES, 4, depth, cols), bf16),
                [pltpu.VMEM((2, LINES, 4, cr, depth), bf16) for _ in range(CHUNKS)],
                pltpu.VMEM((2, LINES, 2, 8, 128), i32),
                [pltpu.VMEM((NOPAIR + 1, cr, cols), f32) for _ in range(2)],
                [pltpu.VMEM((NOSLOT + 1, cr, cols), f32) for _ in range(CHUNKS)],
                [pltpu.VMEM((RING, n_own, cr, cols), f32) for _ in range(CHUNKS)],
                [pltpu.VMEM((2, n_own // 2, cr, cols), f32) for _ in range(CHUNKS)],
                [pltpu.VMEM((2, n_own, cr, cols), f32) for _ in range(CHUNKS)],
                pltpu.VMEM((RING, 8, 128), i32),
                pltpu.VMEM((2, 8, 128), i32),
                pltpu.VMEM((2, n_own, 128), i32),
                pltpu.SMEM((2, 8, 128), i32),
                pltpu.SMEM((2, n_own, 128), i32),
                dma((3,)), dma((n_own // GROUP,)), dma((1 + CHUNKS,)),
                dma((2 + CHUNKS, LINES, 2)), dma((2 + CHUNKS, LINES)),
                dma((2 + CHUNKS,)), dma((2 + CHUNKS,)), dma((2 + CHUNKS,)),
                dma((1,)), dma((RING,)), dma((1,)), dma((1,)),
                dma((CHUNKS,)), dma((CHUNKS, 2, n_own // 2 // GROUP)), dma((CHUNKS, 2, n_own // GROUP)),
            ],
            compiler_params=pltpu.CompilerParams(collective_id=0, has_side_effects=True,
                                                 vmem_limit_bytes=60 * 1024 * 1024),
        )(a, b, pairs, coords, cidx)
        return out[None]

    return jax.shard_map(per_device, mesh=mesh, in_specs=(dev_spec,) * 5, out_specs=dev_spec, check_vma=False)
```

```python
import jax
import jax.numpy as jnp
from jax import lax
from jax.experimental import pallas as pl
from jax.experimental.pallas import tpu as pltpu
from jax.sharding import PartitionSpec as P

RING = 4
PLANE = 32
LINES = PLANE // 2
SLOTS = 8
NOPAIR = 16
NOSLOT = PLANE * SLOTS
ROWS = (64, 64)
B, A, TAB = range(3)
XY, XZ = PASSES = range(2)
OWN, NEXT, FAR, PREV = range(RING)
OTHERS = (FAR, NEXT, PREV)
NEAR = (NEXT, PREV)
CHUNKS = len(ROWS)
FIRST = tuple(sum(ROWS[:ch]) for ch in range(CHUNKS))
GROUP = 4
MESH = pl.DeviceIdType.MESH


def order_of(j):
    return j + (j // 2) * (1 - 2 * (j % 2))


def kernel(a_ref, b_ref, pairs_hbm, coords_hbm, cidx_hbm, out_ref, pairs_ref, coords_ref, cidx_ref, result, held_b,
           held_a, held_t, prods, parts, acc, opp, fin, cb, tblv, selv, tbl_s, sel_s, ints_sem, out_sem, local_sem,
           own_sem, sib_sem, f_sem, s_sem, d_sem, csend_sem, crecv_sem, smem_sem, sel_sem, rs_send, opp_sem, fin_sem):
    me = lax.axis_index("k")
    z = me // PLANE
    y = me % PLANE // 8
    x = me % 8 // 2
    c = me % 2
    n_own = out_ref.shape[0]
    half_own = n_own // 2
    n_grp = half_own // GROUP
    cols = out_ref.shape[2]

    def dev(zz, yy, xx, cc):
        return {"k": ((zz * 4 + yy) * 4 + xx) * 2 + cc}

    sibling = dev(z, y, x, 1 - c)

    def f_dev(p, off):
        if p == 0:
            return dev(z, (y + off * c) % 4, (x + off * (1 - c)) % 4, c)
        return dev(z, y, (x + off) % 4, c)

    def s_dev(p, off):
        if p == 0:
            return dev(z, (y + off * (1 - c)) % 4, (x + off * c) % 4, c)
        return dev((z + off) % 4, y, x, c)

    def r_dev(p, off):
        if p == 0:
            return dev((z + off) % 4, y, x, c)
        return dev(z, (y + off) % 4, x, c)

    def slot_of(p, core, df, ds):
        if p == 0:
            sx = (x + df * (1 - core) + ds * core) % 4
            sy = (y + df * core + ds * (1 - core)) % 4
            return sy * 4 + sx
        return (z + ds) % 4 * 4 + (x + df) % 4

    my_slot = (y * 4 + x, z * 4 + x)
    here = (z, y)
    up, two, down = ([(v + off) % 4 for v in here] for off in (1, 2, 3))

    barrier = pltpu.get_barrier_semaphore()
    for peer in [sibling] + [dev_of(0, off) for dev_of in (f_dev, s_dev, r_dev) for off in OTHERS]:
        pl.semaphore_signal(barrier, inc=1, device_id=peer, device_id_type=MESH)

    held = (held_b, held_a, held_t)
    ints = [pltpu.make_async_copy(src, dst, ints_sem.at[i]) for i, (src, dst) in enumerate(
        ((pairs_hbm, pairs_ref), (coords_hbm, coords_ref), (cidx_hbm, cidx_ref)))]
    loads = []
    for p in (1, 0):
        loads.append(pltpu.make_async_copy(b_ref, held_b[p].at[c, my_slot[p]], local_sem.at[2 * p]))
        loads.append(pltpu.make_async_copy(a_ref.at[:, pl.ds(FIRST[p], ROWS[p])], held_a[p].at[c, my_slot[p]],
                                           local_sem.at[2 * p + 1]))
    for cp in ints + loads:
        cp.start()
    for ref in prods:
        ref[NOPAIR] = jnp.zeros(ref.shape[1:], jnp.float32)
    for ref in parts:
        ref[NOSLOT] = jnp.zeros(ref.shape[1:], jnp.float32)

    for cp in ints:
        cp.wait()

    def block_code(ij):
        return jnp.where(ij[0:1] >= 0, ij[0:1] * 256 + ij[1:2], -1)

    code = block_code(coords_ref[...])
    for h in (0, 1):
        span = pl.ds(128 * h, 128)
        for u in range(4):
            left = pairs_ref[u, 0:1, span]
            pid = jnp.where(left >= 0, left * 4 + pairs_ref[u, 1:2, span], NOPAIR)
            for p in PASSES:
                held_t[p][c, my_slot[p], h, u:u + 1] = pid
        for p in PASSES:
            held_t[p][c, my_slot[p], h, 4:5] = code[:, 128 * h:128 * h + 128]
            held_t[p][c, my_slot[p], h, 5:8] = jnp.zeros((3, 128), jnp.int32)
    for p in PASSES:
        cb[p][here[p]] = jnp.full((8, 128), -2, jnp.int32)
        cb[p][here[p], 0:1, 0:n_own] = block_code(cidx_ref[...])

    pl.semaphore_wait(barrier, 10)

    def whole(p, k, core, slot):
        return held[k][p].at[core, slot]

    def half(p, k, core, slot, h):
        n_half = held[k][p].shape[2] // 2
        return held[k][p].at[core, slot, pl.ds(n_half * h, n_half)]

    def send(ref, target, send_sem, recv_sem):
        pltpu.make_async_remote_copy(src_ref=ref, dst_ref=ref, send_sem=send_sem, recv_sem=recv_sem,
                                     device_id=target, device_id_type=MESH).start()

    def bytes_wait(ref, sem):
        pltpu.make_async_copy(ref, ref, sem).wait()

    def to_sibling(p, k, slot):
        send(whole(p, k, c, slot), sibling, d_sem.at[p, k], sib_sem.at[p, k, slot])

    def to_f(p, k, slot, offs=NEAR):
        for off in offs:
            send(whole(p, k, c, slot), f_dev(p, off), f_sem.at[p, k], own_sem.at[p, k, slot, 0])

    def to_s(p, k, slot, offs=NEAR):
        for off in offs:
            send(whole(p, k, c, slot), s_dev(p, off), s_sem.at[p, k], own_sem.at[p, k, slot, 0])

    def got_whole(p, k, slot):
        bytes_wait(whole(p, k, c, slot), own_sem.at[p, k, slot, 0])

    def got_halves(p, k, slot):
        for h in (0, 1):
            bytes_wait(half(p, k, c, slot, h), own_sem.at[p, k, slot, h])

    def line_near(p, k):
        for df, h, off in ((1, 1, 3), (3, 0, 1)):
            slot = slot_of(p, c, df, 0)
            got_whole(p, k, slot)
            send(half(p, k, c, slot, h), f_dev(p, off), f_sem.at[p, k], own_sem.at[p, k, slot, h])
            to_s(p, k, slot)
            to_sibling(p, k, slot)

    def line_far(p, k):
        slot = slot_of(p, c, 2, 0)
        got_halves(p, k, slot)
        to_s(p, k, slot)
        to_sibling(p, k, slot)

    def side_near(df, p, k):
        for ds, h, off in ((1, 1, 3), (3, 0, 1)):
            slot = slot_of(p, c, df, ds)
            got_whole(p, k, slot)
            send(half(p, k, c, slot, h), s_dev(p, off), s_sem.at[p, k], own_sem.at[p, k, slot, h])
            to_sibling(p, k, slot)

    def side_far(df, p, k):
        slot = slot_of(p, c, df, 2)
        got_halves(p, k, slot)
        to_sibling(p, k, slot)

    def t_line(p, slot):
        to_s(p, TAB, slot, OTHERS)
        to_sibling(p, TAB, slot)

    def t_lines(p):
        for df in (1, 3, 2):
            slot = slot_of(p, c, df, 0)
            got_whole(p, TAB, slot)
            t_line(p, slot)

    def t_sides(p):
        def t_side(n, carry):
            slot = slot_of(p, c, n // 3, 1 + n % 3)
            got_whole(p, TAB, slot)
            to_sibling(p, TAB, slot)
            return carry
        lax.fori_loop(0, 12, t_side, 0)

    for p in PASSES:
        to_f(p, TAB, my_slot[p], OTHERS)
        t_line(p, my_slot[p])
        for off in OTHERS:
            pltpu.make_async_remote_copy(
                src_ref=cb[p].at[here[p]], dst_ref=cb[p].at[here[p]], send_sem=csend_sem.at[p],
                recv_sem=crecv_sem.at[p, here[p]], device_id=r_dev(p, off), device_id_type=MESH).start()
    for i, cp in enumerate(loads):
        p, k = 1 - i // 2, i % 2
        cp.wait()
        to_f(p, k, my_slot[p])
        to_s(p, k, my_slot[p])
        to_sibling(p, k, my_slot[p])

    def lane_of(p, slot, col, r):
        if p == 0:
            return 64 * (col % 2) + 4 * slot + 2 * (col // 2) + r
        return 64 * (slot // 8) + 16 * col + 2 * (slot % 8) + r

    def build_tables(p):
        lane = lax.broadcasted_iota(jnp.int32, (8, 128), 1)
        start = me % PLANE * 2 if p == 0 else z % 2 * 64 + x * 4 + c * 2

        def sib_tables(slot, carry):
            bytes_wait(whole(p, TAB, 1 - c, slot), sib_sem.at[p, TAB, slot])
            return carry

        lax.fori_loop(0, LINES, sib_tables, 0)

        def pick(slot, tables):
            picked = []
            for core, table in enumerate(tables):
                if p == 0:
                    for h in (0, 1):
                        moved = pltpu.roll(held_t[p][core, slot, h], (128 - start + 4 * slot + 2 * h) % 128, 1)
                        table = jnp.where(lane % 64 // 2 == 2 * slot + h, moved, table)
                else:
                    shift = (256 - start + 64 * (slot // 8) + 2 * (slot % 8)) % 128
                    moved = pltpu.roll(held_t[p][core, slot, z // 2], shift, 1)
                    mine = lane // 64 * 8 + lane % 16 // 2 == slot
                    table = jnp.where(mine, moved, table)
                picked.append(table)
            return tuple(picked)

        none = jnp.zeros((8, 128), jnp.int32)
        picked = lax.fori_loop(0, LINES, pick, (none, none), unroll=8)
        for core in (0, 1):
            tblv[p][core] = picked[core]
        sub = lax.broadcasted_iota(jnp.int32, (n_own, 128), 0)
        lane = lax.broadcasted_iota(jnp.int32, (n_own, 128), 1)
        if p == 0:
            slot, col = lane % 64 // 4, 2 * (lane // 2 % 2) + lane // 64
        else:
            slot, col = lane // 64 * 8 + lane % 16 // 2, lane % 64 // 16
        for row in (up[p], two[p], down[p]):
            bytes_wait(cb[p].at[row], crecv_sem.at[p, row])
        wanted = jnp.zeros((n_own, 128), jnp.int32)
        for cc in range(RING):
            column = jnp.where(sub == lane, jnp.broadcast_to(cb[p][cc, 0:1], (n_own, 128)), 0)
            for bit in range(7):
                column = column + pltpu.roll(column, 1 << bit, 1)
            wanted = jnp.where(col == cc, column, wanted)
        for core in (0, 1):
            index = (slot * 2 + core) * SLOTS + 2 * col + lane % 2
            hit = jnp.where(jnp.broadcast_to(picked[core][4:5], (n_own, 128)) == wanted, index - NOSLOT, 0)
            selv[p][core] = NOSLOT + jnp.where(hit != 0, hit, pltpu.roll(hit, 127, 1))

    def smem_copies(p):
        return (pltpu.make_async_copy(tblv[p], tbl_s[p], smem_sem.at[p]),
                pltpu.make_async_copy(selv[p], sel_s[p], sel_sem.at[p]))

    def compute(p, core, slot, prod):
        chunk_rows = ROWS[p]
        span = pl.ds(0, chunk_rows)
        lhs = held_a[p][core, slot].reshape(4 * chunk_rows, -1)
        for pair in (0, 1):
            rhs = jnp.concatenate([held_b[p][core, slot, 2 * pair], held_b[p][core, slot, 2 * pair + 1]], axis=1)
            res = jnp.dot(lhs, rhs, preferred_element_type=jnp.float32)
            for a in range(4):
                for b in (0, 1):
                    prod[a * 4 + 2 * pair + b, span] = res[a * chunk_rows:(a + 1) * chunk_rows, b * cols:(b + 1) * cols]
        src = slot * 2 + core
        for j in range(SLOTS):
            at_lane = lane_of(p, slot, j // 2, j % 2)
            total = prod[tbl_s[p][core, 0, at_lane], span]
            for u in (1, 2, 3):
                total = total + prod[tbl_s[p][core, u, at_lane], span]
            parts[p][src * SLOTS + j] = total.astype(jnp.bfloat16).astype(jnp.float32)

    def both(p, df, ds):
        slot = slot_of(p, 1 - c, df, ds)
        for k in (0, 1):
            bytes_wait(whole(p, k, 1 - c, slot), sib_sem.at[p, k, slot])
        compute(p, c, slot_of(p, c, df, ds), prods[0])
        compute(p, 1 - c, slot, prods[1])

    def loop(n, body):
        def run(j, carry):
            body(j)
            return carry
        lax.fori_loop(0, n, run, 0)

    def block_sum(p, col, t):
        total = jnp.zeros((ROWS[p], cols), jnp.float32)
        for i in range(LINES):
            for core in range(2):
                total = total + parts[p][sel_s[p][core, t, lane_of(p, i, col, 0)]]
        return total

    def r_push(p, col, t, dst, recv, off):
        pltpu.make_async_remote_copy(
            src_ref=acc[p].at[col, pl.ds(t, GROUP)], dst_ref=dst, send_sem=rs_send.at[p], recv_sem=recv,
            device_id=r_dev(p, off), device_id_type=MESH).start()

    def sums(p, g, col_of, high):
        def body(i):
            side = i // GROUP
            t = g * GROUP + i % GROUP + half_own * (side * (1 - high) + (1 - side) * high)
            col = col_of(side)
            acc[p][col, t] = block_sum(p, col, t)
        loop(2 * GROUP, body)

    def beside(p):
        return lambda side: (here[p] + 1 + 2 * side) % RING

    def far(p):
        def body(g):
            t = g * GROUP
            sums(p, g, lambda side: two[p], 0)
            r_push(p, two[p], t, opp[p].at[0, pl.ds(t, GROUP)], opp_sem.at[p, 0, g], 1)
            r_push(p, two[p], t + half_own, opp[p].at[1, pl.ds(t, GROUP)], opp_sem.at[p, 1, g], 3)
        loop(n_grp, body)

    def near(p):
        def body(g):
            t = g * GROUP
            sums(p, g, beside(p), 1)
            r_push(p, up[p], t + half_own, fin[p].at[0, pl.ds(t + half_own, GROUP)], fin_sem.at[p, 0, g + n_grp], 1)
            r_push(p, down[p], t, fin[p].at[1, pl.ds(t, GROUP)], fin_sem.at[p, 1, g], 3)
        loop(n_grp, body)

    def combined(p):
        def body(g):
            t = g * GROUP
            sums(p, g, beside(p), 0)
            for side in range(2):
                bytes_wait(opp[p].at[side, pl.ds(t, GROUP)], opp_sem.at[p, side, g])
            for u in range(GROUP):
                acc[p][up[p], t + u] += opp[p][0, t + u]
                acc[p][down[p], t + half_own + u] += opp[p][1, t + u]
            r_push(p, up[p], t, fin[p].at[0, pl.ds(t, GROUP)], fin_sem.at[p, 0, g], 1)
            r_push(p, down[p], t + half_own, fin[p].at[1, pl.ds(t + half_own, GROUP)], fin_sem.at[p, 1, g + n_grp], 3)
        loop(n_grp, body)

    def mine(p):
        def body(t):
            acc[p][here[p], t] = block_sum(p, here[p], t)
        loop(n_own, body)

    def out_copy(gg):
        span = pl.ds(gg * GROUP, GROUP)
        return pltpu.make_async_copy(result.at[span], out_ref.at[span], out_sem.at[gg])

    def finish(p, last):
        def body(g):
            for gg in (g, g + n_grp):
                t = gg * GROUP
                for side in (0, 1):
                    bytes_wait(fin[p].at[side, pl.ds(t, GROUP)], fin_sem.at[p, side, gg])
                for u in range(GROUP):
                    result[t + u, pl.ds(FIRST[p], ROWS[p])] = (
                        acc[p][here[p], t + u] + (fin[p][0, t + u] + fin[p][1, t + u]))
                if last:
                    out_copy(gg).start()
        loop(n_grp, body)

    def at(n, step, *events):
        @pl.when(n == step)
        def _():
            for event, *args in events:
                event(*args)

    t_lines(XZ)
    t_lines(XY)
    line_near(XZ, B)
    side_near(OWN, XZ, B)
    line_near(XZ, A)
    side_near(OWN, XZ, A)
    side_near(OWN, XY, B)
    line_near(XY, B)
    t_sides(XZ)
    side_near(NEXT, XZ, B)
    side_near(OWN, XY, A)
    line_near(XY, A)
    t_sides(XY)
    line_far(XZ, B)
    line_far(XZ, A)
    build_tables(XY)
    side_near(PREV, XZ, B)
    side_far(OWN, XY, B)
    line_far(XY, B)
    build_tables(XZ)
    for p in PASSES:
        for cp in smem_copies(p):
            cp.start()
    side_far(OWN, XZ, B)
    line_far(XY, A)
    for p in PASSES:
        for cp in smem_copies(p):
            cp.wait()

    def step_a(n):
        df = order_of(n)
        both(XY, df, 0)
        both(XZ, df, 0)
        at(n, 0, (side_near, NEXT, XY, B), (side_near, NEXT, XZ, A))
        at(n, 2, (side_near, PREV, XY, B), (side_near, PREV, XZ, A))
        at(n, 3, (side_far, OWN, XY, A), (side_far, OWN, XZ, A))
    loop(4, step_a)

    def step_b(n):
        df = order_of(n // 2)
        ds = 1 + 2 * (n % 2)
        both(XY, df, ds)
        both(XZ, df, ds)
        at(n, 0, (side_near, NEXT, XY, A))
        at(n, 1, (side_near, PREV, XY, A), (side_far, NEXT, XZ, B))
        at(n, 3, (side_near, FAR, XY, B))
        at(n, 4, (side_near, FAR, XY, A))
        at(n, 5, (side_near, FAR, XZ, B), (side_far, NEXT, XY, B), (side_far, PREV, XY, B), (side_far, NEXT, XY, A), (side_near, FAR, XZ, A))
        at(n, 6, (side_far, PREV, XY, A))
        at(n, 7, (side_far, FAR, XY, B), (side_far, FAR, XY, A))
    loop(8, step_b)

    def step_c(n):
        both(XY, order_of(n), 2)
        at(n, 0, (side_far, PREV, XZ, B))
        at(n, 2, (side_far, NEXT, XZ, A))
    loop(4, step_c)
    far(XY)
    side_far(PREV, XZ, A)
    near(XY)
    side_far(FAR, XZ, B)
    side_far(FAR, XZ, A)

    def step_d(n):
        both(XZ, order_of(n), 2)
    loop(4, step_d)
    far(XZ)
    near(XZ)
    combined(XY)
    combined(XZ)
    mine(XY)
    mine(XZ)
    finish(XY, False)
    finish(XZ, True)

    loop(2 * n_grp, lambda gg: out_copy(gg).wait())
    for p in PASSES:
        for k in (0, 1, TAB):
            bytes_wait(held[k][p].at[0, pl.ds(0, 3)], f_sem.at[p, k])
            bytes_wait(held[k][p].at[0, pl.ds(0, 12)], s_sem.at[p, k])
            bytes_wait(held[k][p].at[0], d_sem.at[p, k])
        bytes_wait(cb[p].at[pl.ds(0, 3)], csend_sem.at[p])
        bytes_wait(acc[p].at[pl.ds(0, 3)], rs_send.at[p])


def solution(mesh):
    dev_spec = P(("batch", "k"))

    def per_device(a_loc, b_loc, pair_loc, coord_loc, cidx_loc):
        a, b = a_loc[0], b_loc[0]
        pairs, coords, cidx = (jnp.swapaxes(v[0], -1, -2) for v in (pair_loc, coord_loc, cidx_loc))
        n_own = cidx.shape[1]
        rows, depth, cols = a.shape[1], a.shape[2], b.shape[2]
        assert rows == sum(ROWS)
        f32, i32, bf16 = jnp.float32, jnp.int32, jnp.bfloat16
        dma = pltpu.SemaphoreType.DMA
        out = pl.pallas_call(
            kernel,
            out_shape=jax.ShapeDtypeStruct((n_own, rows, cols), f32),
            in_specs=[pl.BlockSpec(memory_space=pl.ANY)] * 5,
            out_specs=pl.BlockSpec(memory_space=pl.ANY),
            scratch_shapes=[
                pltpu.VMEM(pairs.shape, i32), pltpu.VMEM(coords.shape, i32), pltpu.VMEM(cidx.shape, i32),
                pltpu.VMEM((n_own, rows, cols), f32),
                [pltpu.VMEM((2, LINES, 4, depth, cols), bf16) for cr in ROWS],
                [pltpu.VMEM((2, LINES, 4, cr, depth), bf16) for cr in ROWS],
                [pltpu.VMEM((2, LINES, 2, 8, 128), i32) for cr in ROWS],
                [pltpu.VMEM((NOPAIR + 1, max(ROWS), cols), f32) for _ in range(2)],
                [pltpu.VMEM((NOSLOT + 1, cr, cols), f32) for cr in ROWS],
                [pltpu.VMEM((RING, n_own, cr, cols), f32) for cr in ROWS],
                [pltpu.VMEM((2, n_own // 2, cr, cols), f32) for cr in ROWS],
                [pltpu.VMEM((2, n_own, cr, cols), f32) for cr in ROWS],
                [pltpu.VMEM((RING, 8, 128), i32) for cr in ROWS],
                [pltpu.VMEM((2, 8, 128), i32) for cr in ROWS],
                [pltpu.VMEM((2, n_own, 128), i32) for cr in ROWS],
                [pltpu.SMEM((2, 8, 128), i32) for cr in ROWS],
                [pltpu.SMEM((2, n_own, 128), i32) for cr in ROWS],
                dma((3,)), dma((n_own // GROUP,)), dma((4,)),
                dma((2, 3, LINES, 2)), dma((2, 3, LINES)),
                dma((2, 3)), dma((2, 3)), dma((2, 3)),
                dma((2,)), dma((2, RING)), dma((2,)), dma((2,)),
                dma((2,)), dma((2, 2, n_own // 2 // GROUP)), dma((2, 2, n_own // GROUP)),
            ],
            compiler_params=pltpu.CompilerParams(collective_id=0, has_side_effects=True,
                                                 vmem_limit_bytes=46 * 1024 * 1024),
        )(*[pltpu.with_memory_space_constraint(v, pltpu.HBM) for v in (a, b, pairs, coords, cidx)])
        return out[None]

    return jax.shard_map(per_device, mesh=mesh, in_specs=(dev_spec,) * 5, out_specs=dev_spec, check_vma=False)
```

```python
import jax
import jax.numpy as jnp
from jax import lax
from jax.experimental import pallas as pl
from jax.experimental.pallas import tpu as pltpu
from jax.sharding import PartitionSpec as P

RING = 4
PLANE = 32
LINES = PLANE // 2
SLOTS = 8
NOPAIR = 16
NOSLOT = PLANE * SLOTS
ROWS = (64, 64)
B, A, TAB = range(3)
XY, XZ = PASSES = range(2)
OWN, NEXT, FAR, PREV = range(RING)
OTHERS = (FAR, NEXT, PREV)
NEAR = (NEXT, PREV)
CHUNKS = len(ROWS)
FIRST = tuple(sum(ROWS[:ch]) for ch in range(CHUNKS))
GROUP = 4
MESH = pl.DeviceIdType.MESH


def order_of(j):
    return j + (j // 2) * (1 - 2 * (j % 2))


def kernel(a_ref, b_ref, pairs_hbm, coords_hbm, cidx_hbm, out_ref, pairs_ref, coords_ref, cidx_ref, result, held_b,
           held_a, held_t, prods, parts, acc, opp, fin, cb, tblv, selv, tbl_s, sel_s, ints_sem, out_sem, local_sem,
           own_sem, sib_sem, f_sem, s_sem, d_sem, csend_sem, crecv_sem, smem_sem, sel_sem, rs_send, opp_sem, fin_sem):
    me = lax.axis_index("k")
    z = me // PLANE
    y = me % PLANE // 8
    x = me % 8 // 2
    c = me % 2
    n_own = out_ref.shape[0]
    half_own = n_own // 2
    n_grp = half_own // GROUP
    cols = out_ref.shape[2]

    def dev(zz, yy, xx, cc):
        return {"k": ((zz * 4 + yy) * 4 + xx) * 2 + cc}

    sibling = dev(z, y, x, 1 - c)

    def f_dev(p, off):
        if p == 0:
            return dev(z, (y + off * c) % 4, (x + off * (1 - c)) % 4, c)
        return dev(z, y, (x + off) % 4, c)

    def s_dev(p, off):
        if p == 0:
            return dev(z, (y + off * (1 - c)) % 4, (x + off * c) % 4, c)
        return dev((z + off) % 4, y, x, c)

    def r_dev(p, off):
        if p == 0:
            return dev((z + off) % 4, y, x, c)
        return dev(z, (y + off) % 4, x, c)

    def slot_of(p, core, df, ds):
        if p == 0:
            sx = (x + df * (1 - core) + ds * core) % 4
            sy = (y + df * core + ds * (1 - core)) % 4
            return sy * 4 + sx
        return (z + ds) % 4 * 4 + (x + df) % 4

    my_slot = (y * 4 + x, z * 4 + x)
    here = (z, y)
    up, two, down = ([(v + off) % 4 for v in here] for off in (1, 2, 3))

    barrier = pltpu.get_barrier_semaphore()
    for peer in [sibling] + [dev_of(0, off) for dev_of in (f_dev, s_dev, r_dev) for off in OTHERS]:
        pl.semaphore_signal(barrier, inc=1, device_id=peer, device_id_type=MESH)

    held = (held_b, held_a, held_t)
    ints = [pltpu.make_async_copy(src, dst, ints_sem.at[i]) for i, (src, dst) in enumerate(
        ((pairs_hbm, pairs_ref), (coords_hbm, coords_ref), (cidx_hbm, cidx_ref)))]
    loads = []
    for p in (1, 0):
        loads.append(pltpu.make_async_copy(b_ref, held_b[p].at[c, my_slot[p]], local_sem.at[2 * p]))
        loads.append(pltpu.make_async_copy(a_ref.at[:, pl.ds(FIRST[p], ROWS[p])], held_a[p].at[c, my_slot[p]],
                                           local_sem.at[2 * p + 1]))
    for cp in ints + loads:
        cp.start()
    for ref in prods:
        ref[NOPAIR] = jnp.zeros(ref.shape[1:], jnp.float32)
    for ref in parts:
        ref[NOSLOT] = jnp.zeros(ref.shape[1:], jnp.float32)

    for cp in ints:
        cp.wait()

    def block_code(ij):
        return jnp.where(ij[0:1] >= 0, ij[0:1] * 256 + ij[1:2], -1)

    code = block_code(coords_ref[...])
    for h in (0, 1):
        span = pl.ds(128 * h, 128)
        for u in range(4):
            left = pairs_ref[u, 0:1, span]
            pid = jnp.where(left >= 0, left * 4 + pairs_ref[u, 1:2, span], NOPAIR)
            for p in PASSES:
                held_t[p][c, my_slot[p], h, u:u + 1] = pid
        for p in PASSES:
            held_t[p][c, my_slot[p], h, 4:5] = code[:, 128 * h:128 * h + 128]
            held_t[p][c, my_slot[p], h, 5:8] = jnp.zeros((3, 128), jnp.int32)
    for p in PASSES:
        cb[p][here[p]] = jnp.full((8, 128), -2, jnp.int32)
        cb[p][here[p], 0:1, 0:n_own] = block_code(cidx_ref[...])

    pl.semaphore_wait(barrier, 10)

    def whole(p, k, core, slot):
        return held[k][p].at[core, slot]

    def half(p, k, core, slot, h):
        n_half = held[k][p].shape[2] // 2
        return held[k][p].at[core, slot, pl.ds(n_half * h, n_half)]

    def send(ref, target, send_sem, recv_sem):
        pltpu.make_async_remote_copy(src_ref=ref, dst_ref=ref, send_sem=send_sem, recv_sem=recv_sem,
                                     device_id=target, device_id_type=MESH).start()

    def bytes_wait(ref, sem):
        pltpu.make_async_copy(ref, ref, sem).wait()

    def to_sibling(p, k, slot):
        send(whole(p, k, c, slot), sibling, d_sem.at[p, k], sib_sem.at[p, k, slot])

    def to_f(p, k, slot, offs=NEAR):
        for off in offs:
            send(whole(p, k, c, slot), f_dev(p, off), f_sem.at[p, k], own_sem.at[p, k, slot, 0])

    def to_s(p, k, slot, offs=NEAR):
        for off in offs:
            send(whole(p, k, c, slot), s_dev(p, off), s_sem.at[p, k], own_sem.at[p, k, slot, 0])

    def got_whole(p, k, slot):
        bytes_wait(whole(p, k, c, slot), own_sem.at[p, k, slot, 0])

    def got_halves(p, k, slot):
        for h in (0, 1):
            bytes_wait(half(p, k, c, slot, h), own_sem.at[p, k, slot, h])

    def line_near(p, k):
        for df, h, off in ((1, 1, 3), (3, 0, 1)):
            slot = slot_of(p, c, df, 0)
            got_whole(p, k, slot)
            send(half(p, k, c, slot, h), f_dev(p, off), f_sem.at[p, k], own_sem.at[p, k, slot, h])
            to_s(p, k, slot)
            to_sibling(p, k, slot)

    def line_far(p, k):
        slot = slot_of(p, c, 2, 0)
        got_halves(p, k, slot)
        to_s(p, k, slot)
        to_sibling(p, k, slot)

    def side_near(df, p, k):
        for ds, h, off in ((1, 1, 3), (3, 0, 1)):
            slot = slot_of(p, c, df, ds)
            got_whole(p, k, slot)
            send(half(p, k, c, slot, h), s_dev(p, off), s_sem.at[p, k], own_sem.at[p, k, slot, h])
            to_sibling(p, k, slot)

    def side_far(df, p, k):
        slot = slot_of(p, c, df, 2)
        got_halves(p, k, slot)
        to_sibling(p, k, slot)

    def t_line(p, slot):
        to_s(p, TAB, slot, OTHERS)
        to_sibling(p, TAB, slot)

    def t_lines(p):
        for df in (1, 3, 2):
            slot = slot_of(p, c, df, 0)
            got_whole(p, TAB, slot)
            t_line(p, slot)

    def t_sides(p):
        def t_side(n, carry):
            slot = slot_of(p, c, n // 3, 1 + n % 3)
            got_whole(p, TAB, slot)
            to_sibling(p, TAB, slot)
            return carry
        lax.fori_loop(0, 12, t_side, 0)

    for p in PASSES:
        to_f(p, TAB, my_slot[p], OTHERS)
        t_line(p, my_slot[p])
        for off in OTHERS:
            pltpu.make_async_remote_copy(
                src_ref=cb[p].at[here[p]], dst_ref=cb[p].at[here[p]], send_sem=csend_sem.at[p],
                recv_sem=crecv_sem.at[p, here[p]], device_id=r_dev(p, off), device_id_type=MESH).start()
    for i, cp in enumerate(loads):
        p, k = 1 - i // 2, i % 2
        cp.wait()
        to_f(p, k, my_slot[p])
        to_s(p, k, my_slot[p])
        to_sibling(p, k, my_slot[p])

    def lane_of(p, slot, col, r):
        if p == 0:
            return 64 * (col % 2) + 4 * slot + 2 * (col // 2) + r
        return 64 * (slot // 8) + 16 * col + 2 * (slot % 8) + r

    def build_tables(p):
        lane = lax.broadcasted_iota(jnp.int32, (8, 128), 1)
        start = me % PLANE * 2 if p == 0 else z % 2 * 64 + x * 4 + c * 2

        def sib_tables(slot, carry):
            bytes_wait(whole(p, TAB, 1 - c, slot), sib_sem.at[p, TAB, slot])
            return carry

        lax.fori_loop(0, LINES, sib_tables, 0)

        def pick(slot, tables):
            picked = []
            for core, table in enumerate(tables):
                if p == 0:
                    for h in (0, 1):
                        moved = pltpu.roll(held_t[p][core, slot, h], (128 - start + 4 * slot + 2 * h) % 128, 1)
                        table = jnp.where(lane % 64 // 2 == 2 * slot + h, moved, table)
                else:
                    shift = (256 - start + 64 * (slot // 8) + 2 * (slot % 8)) % 128
                    moved = pltpu.roll(held_t[p][core, slot, z // 2], shift, 1)
                    mine = lane // 64 * 8 + lane % 16 // 2 == slot
                    table = jnp.where(mine, moved, table)
                picked.append(table)
            return tuple(picked)

        none = jnp.zeros((8, 128), jnp.int32)
        picked = lax.fori_loop(0, LINES, pick, (none, none), unroll=4)
        for core in (0, 1):
            tblv[p][core] = picked[core]
        sub = lax.broadcasted_iota(jnp.int32, (n_own, 128), 0)
        lane = lax.broadcasted_iota(jnp.int32, (n_own, 128), 1)
        if p == 0:
            slot, col = lane % 64 // 4, 2 * (lane // 2 % 2) + lane // 64
        else:
            slot, col = lane // 64 * 8 + lane % 16 // 2, lane % 64 // 16
        for row in (up[p], two[p], down[p]):
            bytes_wait(cb[p].at[row], crecv_sem.at[p, row])
        wanted = jnp.zeros((n_own, 128), jnp.int32)
        for cc in range(RING):
            column = jnp.where(sub == lane, jnp.broadcast_to(cb[p][cc, 0:1], (n_own, 128)), 0)
            for bit in range(7):
                column = column + pltpu.roll(column, 1 << bit, 1)
            wanted = jnp.where(col == cc, column, wanted)
        for core in (0, 1):
            index = (slot * 2 + core) * SLOTS + 2 * col + lane % 2
            hit = jnp.where(jnp.broadcast_to(picked[core][4:5], (n_own, 128)) == wanted, index - NOSLOT, 0)
            selv[p][core] = NOSLOT + jnp.where(hit != 0, hit, pltpu.roll(hit, 127, 1))

    def smem_copies(p):
        return (pltpu.make_async_copy(tblv[p], tbl_s[p], smem_sem.at[p]),
                pltpu.make_async_copy(selv[p], sel_s[p], sel_sem.at[p]))

    def compute(p, core, slot, prod):
        chunk_rows = ROWS[p]
        span = pl.ds(0, chunk_rows)
        lhs = held_a[p][core, slot].reshape(4 * chunk_rows, -1)
        for pair in (0, 1):
            rhs = jnp.concatenate([held_b[p][core, slot, 2 * pair], held_b[p][core, slot, 2 * pair + 1]], axis=1)
            res = jnp.dot(lhs, rhs, preferred_element_type=jnp.float32)
            for a in range(4):
                for b in (0, 1):
                    prod[a * 4 + 2 * pair + b, span] = res[a * chunk_rows:(a + 1) * chunk_rows, b * cols:(b + 1) * cols]
        src = slot * 2 + core
        for j in range(SLOTS):
            at_lane = lane_of(p, slot, j // 2, j % 2)
            total = prod[tbl_s[p][core, 0, at_lane], span]
            for u in (1, 2, 3):
                total = total + prod[tbl_s[p][core, u, at_lane], span]
            parts[p][src * SLOTS + j] = total.astype(jnp.bfloat16).astype(jnp.float32)

    def both(p, df, ds):
        slot = slot_of(p, 1 - c, df, ds)
        for k in (0, 1):
            bytes_wait(whole(p, k, 1 - c, slot), sib_sem.at[p, k, slot])
        compute(p, c, slot_of(p, c, df, ds), prods[0])
        compute(p, 1 - c, slot, prods[1])

    def loop(n, body):
        def run(j, carry):
            body(j)
            return carry
        lax.fori_loop(0, n, run, 0)

    def block_sum(p, col, t):
        total = jnp.zeros((ROWS[p], cols), jnp.float32)
        for i in range(LINES):
            for core in range(2):
                total = total + parts[p][sel_s[p][core, t, lane_of(p, i, col, 0)]]
        return total

    def r_push(p, col, t, dst, recv, off):
        pltpu.make_async_remote_copy(
            src_ref=acc[p].at[col, pl.ds(t, GROUP)], dst_ref=dst, send_sem=rs_send.at[p], recv_sem=recv,
            device_id=r_dev(p, off), device_id_type=MESH).start()

    def sums(p, g, col_of, high):
        def body(i):
            side = i // GROUP
            t = g * GROUP + i % GROUP + half_own * (side * (1 - high) + (1 - side) * high)
            col = col_of(side)
            acc[p][col, t] = block_sum(p, col, t)
        loop(2 * GROUP, body)

    def beside(p):
        return lambda side: (here[p] + 1 + 2 * side) % RING

    def far(p):
        def body(g):
            t = g * GROUP
            sums(p, g, lambda side: two[p], 0)
            r_push(p, two[p], t, opp[p].at[0, pl.ds(t, GROUP)], opp_sem.at[p, 0, g], 1)
            r_push(p, two[p], t + half_own, opp[p].at[1, pl.ds(t, GROUP)], opp_sem.at[p, 1, g], 3)
        loop(n_grp, body)

    def near(p):
        def body(g):
            t = g * GROUP
            sums(p, g, beside(p), 1)
            r_push(p, up[p], t + half_own, fin[p].at[0, pl.ds(t + half_own, GROUP)], fin_sem.at[p, 0, g + n_grp], 1)
            r_push(p, down[p], t, fin[p].at[1, pl.ds(t, GROUP)], fin_sem.at[p, 1, g], 3)
        loop(n_grp, body)

    def combined(p):
        def body(g):
            t = g * GROUP
            sums(p, g, beside(p), 0)
            for side in range(2):
                bytes_wait(opp[p].at[side, pl.ds(t, GROUP)], opp_sem.at[p, side, g])
            for u in range(GROUP):
                acc[p][up[p], t + u] += opp[p][0, t + u]
                acc[p][down[p], t + half_own + u] += opp[p][1, t + u]
            r_push(p, up[p], t, fin[p].at[0, pl.ds(t, GROUP)], fin_sem.at[p, 0, g], 1)
            r_push(p, down[p], t + half_own, fin[p].at[1, pl.ds(t + half_own, GROUP)], fin_sem.at[p, 1, g + n_grp], 3)
        loop(n_grp, body)

    def mine(p):
        def body(t):
            acc[p][here[p], t] = block_sum(p, here[p], t)
        loop(n_own, body)

    def out_copy(gg):
        span = pl.ds(gg * GROUP, GROUP)
        return pltpu.make_async_copy(result.at[span], out_ref.at[span], out_sem.at[gg])

    def finish(p, last):
        def body(g):
            for gg in (g, g + n_grp):
                t = gg * GROUP
                for side in (0, 1):
                    bytes_wait(fin[p].at[side, pl.ds(t, GROUP)], fin_sem.at[p, side, gg])
                for u in range(GROUP):
                    result[t + u, pl.ds(FIRST[p], ROWS[p])] = (
                        acc[p][here[p], t + u] + (fin[p][0, t + u] + fin[p][1, t + u]))
                if last:
                    out_copy(gg).start()
        loop(n_grp, body)

    def at(n, step, *events):
        @pl.when(n == step)
        def _():
            for event, *args in events:
                event(*args)

    t_lines(XZ)
    t_lines(XY)
    line_near(XZ, B)
    side_near(OWN, XZ, B)
    line_near(XZ, A)
    side_near(OWN, XZ, A)
    side_near(OWN, XY, B)
    line_near(XY, B)
    t_sides(XZ)
    side_near(NEXT, XZ, B)
    side_near(OWN, XY, A)
    line_near(XY, A)
    build_tables(XZ)
    t_sides(XY)
    line_far(XZ, B)
    line_far(XZ, A)
    build_tables(XY)
    for p in PASSES:
        for cp in smem_copies(p):
            cp.start()
    side_near(PREV, XZ, B)
    side_far(OWN, XY, B)
    line_far(XY, B)
    side_far(OWN, XZ, B)
    line_far(XY, A)
    for p in PASSES:
        for cp in smem_copies(p):
            cp.wait()

    def step_a(n):
        df = order_of(n)
        both(XY, df, 0)
        at(n, 0, (side_near, NEXT, XY, B), (side_near, NEXT, XZ, A))
        at(n, 2, (side_near, PREV, XY, B), (side_near, PREV, XZ, A))
        at(n, 3, (side_far, OWN, XY, A), (side_far, OWN, XZ, A))
        both(XZ, df, 0)
    loop(4, step_a)

    def step_b(n):
        df = order_of(n // 2)
        ds = 1 + 2 * (n % 2)
        both(XY, df, ds)
        at(n, 0, (side_near, NEXT, XY, A))
        at(n, 1, (side_near, PREV, XY, A), (side_far, NEXT, XZ, B))
        at(n, 3, (side_near, FAR, XY, B))
        at(n, 4, (side_near, FAR, XY, A))
        at(n, 5, (side_near, FAR, XZ, B), (side_far, NEXT, XY, B), (side_far, PREV, XY, B), (side_far, NEXT, XY, A), (side_near, FAR, XZ, A))
        at(n, 6, (side_far, PREV, XY, A))
        at(n, 7, (side_far, FAR, XY, B), (side_far, FAR, XY, A))
        both(XZ, df, ds)
    loop(8, step_b)

    def step_c(n):
        both(XY, order_of(n), 2)
        at(n, 0, (side_far, PREV, XZ, B))
        at(n, 2, (side_far, NEXT, XZ, A))
    loop(4, step_c)
    far(XY)
    side_far(PREV, XZ, A)

    def step_d(n):
        at(n, 2, (side_far, FAR, XZ, B))
        at(n, 3, (side_far, FAR, XZ, A))
        both(XZ, order_of(n), 2)
    loop(RING, step_d)
    far(XZ)
    near(XZ)
    near(XY)
    combined(XY)
    combined(XZ)
    mine(XY)
    mine(XZ)
    finish(XY, False)
    finish(XZ, True)

    loop(2 * n_grp, lambda gg: out_copy(gg).wait())
    for p in PASSES:
        for k in (0, 1, TAB):
            bytes_wait(held[k][p].at[0, pl.ds(0, 3)], f_sem.at[p, k])
            bytes_wait(held[k][p].at[0, pl.ds(0, 12)], s_sem.at[p, k])
            bytes_wait(held[k][p].at[0], d_sem.at[p, k])
        bytes_wait(cb[p].at[pl.ds(0, 3)], csend_sem.at[p])
        bytes_wait(acc[p].at[pl.ds(0, 3)], rs_send.at[p])


def solution(mesh):
    dev_spec = P(("batch", "k"))

    def per_device(a_loc, b_loc, pair_loc, coord_loc, cidx_loc):
        a, b = a_loc[0], b_loc[0]
        pairs, coords, cidx = (jnp.swapaxes(v[0], -1, -2) for v in (pair_loc, coord_loc, cidx_loc))
        n_own = cidx.shape[1]
        rows, depth, cols = a.shape[1], a.shape[2], b.shape[2]
        assert rows == sum(ROWS)
        f32, i32, bf16 = jnp.float32, jnp.int32, jnp.bfloat16
        dma = pltpu.SemaphoreType.DMA
        out = pl.pallas_call(
            kernel,
            out_shape=jax.ShapeDtypeStruct((n_own, rows, cols), f32),
            in_specs=[pl.BlockSpec(memory_space=pl.ANY)] * 5,
            out_specs=pl.BlockSpec(memory_space=pl.ANY),
            scratch_shapes=[
                pltpu.VMEM(pairs.shape, i32), pltpu.VMEM(coords.shape, i32), pltpu.VMEM(cidx.shape, i32),
                pltpu.VMEM((n_own, rows, cols), f32),
                [pltpu.VMEM((2, LINES, 4, depth, cols), bf16) for cr in ROWS],
                [pltpu.VMEM((2, LINES, 4, cr, depth), bf16) for cr in ROWS],
                [pltpu.VMEM((2, LINES, 2, 8, 128), i32) for cr in ROWS],
                [pltpu.VMEM((NOPAIR + 1, max(ROWS), cols), f32) for _ in range(2)],
                [pltpu.VMEM((NOSLOT + 1, cr, cols), f32) for cr in ROWS],
                [pltpu.VMEM((RING, n_own, cr, cols), f32) for cr in ROWS],
                [pltpu.VMEM((2, n_own // 2, cr, cols), f32) for cr in ROWS],
                [pltpu.VMEM((2, n_own, cr, cols), f32) for cr in ROWS],
                [pltpu.VMEM((RING, 8, 128), i32) for cr in ROWS],
                [pltpu.VMEM((2, 8, 128), i32) for cr in ROWS],
                [pltpu.VMEM((2, n_own, 128), i32) for cr in ROWS],
                [pltpu.SMEM((2, 8, 128), i32) for cr in ROWS],
                [pltpu.SMEM((2, n_own, 128), i32) for cr in ROWS],
                dma((3,)), dma((n_own // GROUP,)), dma((4,)),
                dma((2, 3, LINES, 2)), dma((2, 3, LINES)),
                dma((2, 3)), dma((2, 3)), dma((2, 3)),
                dma((2,)), dma((2, RING)), dma((2,)), dma((2,)),
                dma((2,)), dma((2, 2, n_own // 2 // GROUP)), dma((2, 2, n_own // GROUP)),
            ],
            compiler_params=pltpu.CompilerParams(collective_id=0, has_side_effects=True,
                                                 vmem_limit_bytes=46 * 1024 * 1024),
        )(*[pltpu.with_memory_space_constraint(v, pltpu.HBM) for v in (a, b, pairs, coords, cidx)])
        return out[None]

    return jax.shard_map(per_device, mesh=mesh, in_specs=(dev_spec,) * 5, out_specs=dev_spec, check_vma=False)
```

```python
import jax
import jax.numpy as jnp
from jax import lax
from jax.experimental import pallas as pl
from jax.experimental.pallas import tpu as pltpu
from jax.sharding import PartitionSpec as P

RING = 4
PLANE = 32
LINES = PLANE // 2
SLOTS = 8
NOPAIR = 16
NOSLOT = PLANE * SLOTS
ROWS = (64, 64)
B, A, TAB = range(3)
XY, XZ = PASSES = range(2)
OWN, NEXT, FAR, PREV = range(RING)
OTHERS = (FAR, NEXT, PREV)
NEAR = (NEXT, PREV)
CHUNKS = len(ROWS)
FIRST = tuple(sum(ROWS[:ch]) for ch in range(CHUNKS))
GROUP = 4
MESH = pl.DeviceIdType.MESH


def order_of(j):
    return j + (j // 2) * (1 - 2 * (j % 2))


def kernel(a_ref, b_ref, pairs_hbm, coords_hbm, cidx_hbm, out_ref, pairs_ref, coords_ref, cidx_ref, result, held_b,
           held_a, held_t, prods, parts, acc, opp, fin, cb, tblv, selv, tbl_s, sel_s, ints_sem, out_sem, local_sem,
           own_sem, sib_sem, f_sem, s_sem, d_sem, csend_sem, crecv_sem, smem_sem, sel_sem, rs_send, opp_sem, fin_sem):
    me = lax.axis_index("k")
    z = me // PLANE
    y = me % PLANE // 8
    x = me % 8 // 2
    c = me % 2
    n_own = out_ref.shape[0]
    half_own = n_own // 2
    n_grp = half_own // GROUP
    cols = out_ref.shape[2]

    def dev(zz, yy, xx, cc):
        return {"k": ((zz * 4 + yy) * 4 + xx) * 2 + cc}

    sibling = dev(z, y, x, 1 - c)

    def f_dev(p, off):
        if p == 0:
            return dev(z, (y + off * c) % 4, (x + off * (1 - c)) % 4, c)
        return dev(z, y, (x + off) % 4, c)

    def s_dev(p, off):
        if p == 0:
            return dev(z, (y + off * (1 - c)) % 4, (x + off * c) % 4, c)
        return dev((z + off) % 4, y, x, c)

    def r_dev(p, off):
        if p == 0:
            return dev((z + off) % 4, y, x, c)
        return dev(z, (y + off) % 4, x, c)

    def slot_of(p, core, df, ds):
        if p == 0:
            sx = (x + df * (1 - core) + ds * core) % 4
            sy = (y + df * core + ds * (1 - core)) % 4
            return sy * 4 + sx
        return (z + ds) % 4 * 4 + (x + df) % 4

    my_slot = (y * 4 + x, z * 4 + x)
    here = (z, y)
    up, two, down = ([(v + off) % 4 for v in here] for off in (1, 2, 3))

    barrier = pltpu.get_barrier_semaphore()
    for peer in [sibling] + [dev_of(0, off) for dev_of in (f_dev, s_dev, r_dev) for off in OTHERS]:
        pl.semaphore_signal(barrier, inc=1, device_id=peer, device_id_type=MESH)

    held = (held_b, held_a, held_t)
    ints = [pltpu.make_async_copy(src, dst, ints_sem.at[i]) for i, (src, dst) in enumerate(
        ((pairs_hbm, pairs_ref), (coords_hbm, coords_ref), (cidx_hbm, cidx_ref)))]
    loads = []
    for p in (1, 0):
        loads.append(pltpu.make_async_copy(b_ref, held_b[p].at[c, my_slot[p]], local_sem.at[2 * p]))
        loads.append(pltpu.make_async_copy(a_ref.at[:, pl.ds(FIRST[p], ROWS[p])], held_a[p].at[c, my_slot[p]],
                                           local_sem.at[2 * p + 1]))
    for cp in ints + loads:
        cp.start()
    for ref in prods:
        ref[NOPAIR] = jnp.zeros(ref.shape[1:], jnp.float32)
    for ref in parts:
        ref[NOSLOT] = jnp.zeros(ref.shape[1:], jnp.float32)

    for cp in ints:
        cp.wait()

    def block_code(ij):
        return jnp.where(ij[0:1] >= 0, ij[0:1] * 256 + ij[1:2], -1)

    code = block_code(coords_ref[...])
    for h in (0, 1):
        span = pl.ds(128 * h, 128)
        for u in range(4):
            left = pairs_ref[u, 0:1, span]
            pid = jnp.where(left >= 0, left * 4 + pairs_ref[u, 1:2, span], NOPAIR)
            for p in PASSES:
                held_t[p][c, my_slot[p], h, u:u + 1] = pid
        for p in PASSES:
            held_t[p][c, my_slot[p], h, 4:5] = code[:, 128 * h:128 * h + 128]
            held_t[p][c, my_slot[p], h, 5:8] = jnp.zeros((3, 128), jnp.int32)
    for p in PASSES:
        cb[p][here[p]] = jnp.full((8, 128), -2, jnp.int32)
        cb[p][here[p], 0:1, 0:n_own] = block_code(cidx_ref[...])

    pl.semaphore_wait(barrier, 10)

    def whole(p, k, core, slot):
        return held[k][p].at[core, slot]

    def half(p, k, core, slot, h):
        n_half = held[k][p].shape[2] // 2
        return held[k][p].at[core, slot, pl.ds(n_half * h, n_half)]

    def send(ref, target, send_sem, recv_sem):
        pltpu.make_async_remote_copy(src_ref=ref, dst_ref=ref, send_sem=send_sem, recv_sem=recv_sem,
                                     device_id=target, device_id_type=MESH).start()

    def bytes_wait(ref, sem):
        pltpu.make_async_copy(ref, ref, sem).wait()

    def to_sibling(p, k, slot):
        send(whole(p, k, c, slot), sibling, d_sem.at[p, k], sib_sem.at[p, k, slot])

    def to_f(p, k, slot, offs=NEAR):
        for off in offs:
            send(whole(p, k, c, slot), f_dev(p, off), f_sem.at[p, k], own_sem.at[p, k, slot, 0])

    def to_s(p, k, slot, offs=NEAR):
        for off in offs:
            send(whole(p, k, c, slot), s_dev(p, off), s_sem.at[p, k], own_sem.at[p, k, slot, 0])

    def got_whole(p, k, slot):
        bytes_wait(whole(p, k, c, slot), own_sem.at[p, k, slot, 0])

    def got_halves(p, k, slot):
        for h in (0, 1):
            bytes_wait(half(p, k, c, slot, h), own_sem.at[p, k, slot, h])

    def line_near(p, k):
        for df, h, off in ((1, 1, 3), (3, 0, 1)):
            slot = slot_of(p, c, df, 0)
            got_whole(p, k, slot)
            send(half(p, k, c, slot, h), f_dev(p, off), f_sem.at[p, k], own_sem.at[p, k, slot, h])
            to_s(p, k, slot)
            to_sibling(p, k, slot)

    def line_far(p, k):
        slot = slot_of(p, c, 2, 0)
        got_halves(p, k, slot)
        to_s(p, k, slot)
        to_sibling(p, k, slot)

    def side_near(df, p, k):
        for ds, h, off in ((1, 1, 3), (3, 0, 1)):
            slot = slot_of(p, c, df, ds)
            got_whole(p, k, slot)
            send(half(p, k, c, slot, h), s_dev(p, off), s_sem.at[p, k], own_sem.at[p, k, slot, h])
            to_sibling(p, k, slot)

    def side_far(df, p, k):
        slot = slot_of(p, c, df, 2)
        got_halves(p, k, slot)
        to_sibling(p, k, slot)

    def t_line(p, slot):
        to_s(p, TAB, slot, OTHERS)
        to_sibling(p, TAB, slot)

    def t_lines(p):
        for df in (1, 3, 2):
            slot = slot_of(p, c, df, 0)
            got_whole(p, TAB, slot)
            t_line(p, slot)

    def t_sides(p):
        def t_side(n, carry):
            slot = slot_of(p, c, n // 3, 1 + n % 3)
            got_whole(p, TAB, slot)
            to_sibling(p, TAB, slot)
            return carry
        lax.fori_loop(0, 12, t_side, 0)

    for p in PASSES:
        to_f(p, TAB, my_slot[p], OTHERS)
        t_line(p, my_slot[p])
        for off in OTHERS:
            pltpu.make_async_remote_copy(
                src_ref=cb[p].at[here[p]], dst_ref=cb[p].at[here[p]], send_sem=csend_sem.at[p],
                recv_sem=crecv_sem.at[p, here[p]], device_id=r_dev(p, off), device_id_type=MESH).start()
    for i, cp in enumerate(loads):
        p, k = 1 - i // 2, i % 2
        cp.wait()
        to_f(p, k, my_slot[p])
        to_s(p, k, my_slot[p])
        to_sibling(p, k, my_slot[p])

    def lane_of(p, slot, col, r):
        if p == 0:
            return 64 * (col % 2) + 4 * slot + 2 * (col // 2) + r
        return 64 * (slot // 8) + 16 * col + 2 * (slot % 8) + r

    def build_tables(p):
        lane = lax.broadcasted_iota(jnp.int32, (8, 128), 1)
        start = me % PLANE * 2 if p == 0 else z % 2 * 64 + x * 4 + c * 2

        def sib_tables(slot, carry):
            bytes_wait(whole(p, TAB, 1 - c, slot), sib_sem.at[p, TAB, slot])
            return carry

        lax.fori_loop(0, LINES, sib_tables, 0)

        def pick(slot, tables):
            picked = []
            for core, table in enumerate(tables):
                if p == 0:
                    for h in (0, 1):
                        moved = pltpu.roll(held_t[p][core, slot, h], (128 - start + 4 * slot + 2 * h) % 128, 1)
                        table = jnp.where(lane % 64 // 2 == 2 * slot + h, moved, table)
                else:
                    shift = (256 - start + 64 * (slot // 8) + 2 * (slot % 8)) % 128
                    moved = pltpu.roll(held_t[p][core, slot, z // 2], shift, 1)
                    mine = lane // 64 * 8 + lane % 16 // 2 == slot
                    table = jnp.where(mine, moved, table)
                picked.append(table)
            return tuple(picked)

        none = jnp.zeros((8, 128), jnp.int32)
        picked = lax.fori_loop(0, LINES, pick, (none, none), unroll=4)
        for core in (0, 1):
            tblv[p][core] = picked[core]
        sub = lax.broadcasted_iota(jnp.int32, (n_own, 128), 0)
        lane = lax.broadcasted_iota(jnp.int32, (n_own, 128), 1)
        if p == 0:
            slot, col = lane % 64 // 4, 2 * (lane // 2 % 2) + lane // 64
        else:
            slot, col = lane // 64 * 8 + lane % 16 // 2, lane % 64 // 16
        for row in (up[p], two[p], down[p]):
            bytes_wait(cb[p].at[row], crecv_sem.at[p, row])
        wanted = jnp.zeros((n_own, 128), jnp.int32)
        for cc in range(RING):
            column = jnp.where(sub == lane, jnp.broadcast_to(cb[p][cc, 0:1], (n_own, 128)), 0)
            for bit in range(7):
                column = column + pltpu.roll(column, 1 << bit, 1)
            wanted = jnp.where(col == cc, column, wanted)
        for core in (0, 1):
            index = (slot * 2 + core) * SLOTS + 2 * col + lane % 2
            hit = jnp.where(jnp.broadcast_to(picked[core][4:5], (n_own, 128)) == wanted, index - NOSLOT, 0)
            selv[p][core] = NOSLOT + jnp.where(hit != 0, hit, pltpu.roll(hit, 127, 1))

    def smem_copies(p):
        return (pltpu.make_async_copy(tblv[p], tbl_s[p], smem_sem.at[p]),
                pltpu.make_async_copy(selv[p], sel_s[p], sel_sem.at[p]))

    def compute(p, core, slot, prod):
        chunk_rows = ROWS[p]
        span = pl.ds(0, chunk_rows)
        lhs = held_a[p][core, slot].reshape(4 * chunk_rows, -1)
        for pair in (0, 1):
            rhs = jnp.concatenate([held_b[p][core, slot, 2 * pair], held_b[p][core, slot, 2 * pair + 1]], axis=1)
            res = jnp.dot(lhs, rhs, preferred_element_type=jnp.float32)
            for a in range(4):
                for b in (0, 1):
                    prod[a * 4 + 2 * pair + b, span] = res[a * chunk_rows:(a + 1) * chunk_rows, b * cols:(b + 1) * cols]
        src = slot * 2 + core
        for j in range(SLOTS):
            at_lane = lane_of(p, slot, j // 2, j % 2)
            total = prod[tbl_s[p][core, 0, at_lane], span]
            for u in (1, 2, 3):
                total = total + prod[tbl_s[p][core, u, at_lane], span]
            parts[p][src * SLOTS + j] = total.astype(jnp.bfloat16).astype(jnp.float32)

    def products(todo, ds):
        for p, df in todo:
            slot = slot_of(p, 1 - c, df, ds)
            for k in (B, A):
                bytes_wait(whole(p, k, 1 - c, slot), sib_sem.at[p, k, slot])
        for i, (p, df) in enumerate(todo):
            compute(p, c, slot_of(p, c, df, ds), prods[2 * i])
            compute(p, 1 - c, slot_of(p, 1 - c, df, ds), prods[2 * i + 1])

    def loop(n, body):
        def run(j, carry):
            body(j)
            return carry
        lax.fori_loop(0, n, run, 0)

    def block_sum(p, col, t):
        total = jnp.zeros((ROWS[p], cols), jnp.float32)
        for i in range(LINES):
            for core in range(2):
                total = total + parts[p][sel_s[p][core, t, lane_of(p, i, col, 0)]]
        return total

    def r_push(p, col, t, dst, recv, off):
        pltpu.make_async_remote_copy(
            src_ref=acc[p].at[col, pl.ds(t, GROUP)], dst_ref=dst, send_sem=rs_send.at[p], recv_sem=recv,
            device_id=r_dev(p, off), device_id_type=MESH).start()

    def sums(p, g, col_of, high):
        def body(i):
            side = i // GROUP
            t = g * GROUP + i % GROUP + half_own * (side * (1 - high) + (1 - side) * high)
            col = col_of(side)
            acc[p][col, t] = block_sum(p, col, t)
        loop(2 * GROUP, body)

    def beside(p):
        return lambda side: (here[p] + 1 + 2 * side) % RING

    def far(p):
        def body(g):
            t = g * GROUP
            sums(p, g, lambda side: two[p], 0)
            r_push(p, two[p], t, opp[p].at[0, pl.ds(t, GROUP)], opp_sem.at[p, 0, g], 1)
            r_push(p, two[p], t + half_own, opp[p].at[1, pl.ds(t, GROUP)], opp_sem.at[p, 1, g], 3)
        loop(n_grp, body)

    def near(p):
        def body(g):
            t = g * GROUP
            sums(p, g, beside(p), 1)
            r_push(p, up[p], t + half_own, fin[p].at[0, pl.ds(t + half_own, GROUP)], fin_sem.at[p, 0, g + n_grp], 1)
            r_push(p, down[p], t, fin[p].at[1, pl.ds(t, GROUP)], fin_sem.at[p, 1, g], 3)
        loop(n_grp, body)

    def combined(p):
        def body(g):
            t = g * GROUP
            sums(p, g, beside(p), 0)
            for side in range(2):
                bytes_wait(opp[p].at[side, pl.ds(t, GROUP)], opp_sem.at[p, side, g])
            for u in range(GROUP):
                acc[p][up[p], t + u] += opp[p][0, t + u]
                acc[p][down[p], t + half_own + u] += opp[p][1, t + u]
            r_push(p, up[p], t, fin[p].at[0, pl.ds(t, GROUP)], fin_sem.at[p, 0, g], 1)
            r_push(p, down[p], t + half_own, fin[p].at[1, pl.ds(t + half_own, GROUP)], fin_sem.at[p, 1, g + n_grp], 3)
        loop(n_grp, body)

    def mine(p):
        def body(t):
            acc[p][here[p], t] = block_sum(p, here[p], t)
        loop(n_own, body)

    def out_copy(gg):
        span = pl.ds(gg * GROUP, GROUP)
        return pltpu.make_async_copy(result.at[span], out_ref.at[span], out_sem.at[gg])

    def finish(p, last):
        def body(g):
            for gg in (g, g + n_grp):
                t = gg * GROUP
                for side in (0, 1):
                    bytes_wait(fin[p].at[side, pl.ds(t, GROUP)], fin_sem.at[p, side, gg])
                for u in range(GROUP):
                    result[t + u, pl.ds(FIRST[p], ROWS[p])] = (
                        acc[p][here[p], t + u] + (fin[p][0, t + u] + fin[p][1, t + u]))
                if last:
                    out_copy(gg).start()
        loop(n_grp, body)

    def at(n, step, *events):
        @pl.when(n == step)
        def _():
            for event, *args in events:
                event(*args)

    t_lines(XZ)
    t_lines(XY)
    line_near(XZ, B)
    side_near(OWN, XZ, B)
    line_near(XZ, A)
    side_near(OWN, XZ, A)
    side_near(OWN, XY, B)
    line_near(XY, B)
    t_sides(XZ)
    side_near(NEXT, XZ, B)
    side_near(OWN, XY, A)
    line_near(XY, A)
    build_tables(XZ)
    t_sides(XY)
    line_far(XZ, B)
    line_far(XZ, A)
    build_tables(XY)
    for p in PASSES:
        for cp in smem_copies(p):
            cp.start()
    side_near(PREV, XZ, B)
    side_far(OWN, XY, B)
    line_far(XY, B)
    side_far(OWN, XZ, B)
    line_far(XY, A)
    for p in PASSES:
        for cp in smem_copies(p):
            cp.wait()

    def step_a(n):
        df = order_of(n)
        products([(p, df) for p in PASSES], 0)
        at(n, 0, (side_near, NEXT, XY, B), (side_near, NEXT, XZ, A))
        at(n, 2, (side_near, PREV, XY, B), (side_near, PREV, XZ, A))
        at(n, 3, (side_far, OWN, XY, A), (side_far, OWN, XZ, A))
    loop(4, step_a)

    def step_b(n):
        df = order_of(n // 2)
        ds = 1 + 2 * (n % 2)
        products([(p, df) for p in PASSES], ds)
        at(n, 0, (side_near, NEXT, XY, A))
        at(n, 1, (side_near, PREV, XY, A), (side_far, NEXT, XZ, B))
        at(n, 3, (side_near, FAR, XY, B))
        at(n, 4, (side_near, FAR, XY, A))
        at(n, 5, (side_near, FAR, XZ, B), (side_far, NEXT, XY, B), (side_far, PREV, XY, B), (side_far, NEXT, XY, A), (side_near, FAR, XZ, A))
        at(n, 6, (side_far, PREV, XY, A))
        at(n, 7, (side_far, FAR, XY, B), (side_far, FAR, XY, A))
    loop(8, step_b)

    def step_c(n):
        at(n, 0, (side_far, PREV, XZ, B))
        products([(XY, order_of(2 * n + i)) for i in range(2)], FAR)
        at(n, 0, (side_far, NEXT, XZ, A))
    loop(2, step_c)
    far(XY)
    side_far(PREV, XZ, A)

    def step_d(n):
        at(n, 1, (side_far, FAR, XZ, B), (side_far, FAR, XZ, A))
        products([(XZ, order_of(2 * n + i)) for i in range(2)], FAR)
    loop(2, step_d)
    far(XZ)
    near(XZ)
    near(XY)
    combined(XY)
    combined(XZ)
    mine(XY)
    mine(XZ)
    finish(XY, False)
    finish(XZ, True)

    loop(2 * n_grp, lambda gg: out_copy(gg).wait())
    for p in PASSES:
        for k in (0, 1, TAB):
            bytes_wait(held[k][p].at[0, pl.ds(0, 3)], f_sem.at[p, k])
            bytes_wait(held[k][p].at[0, pl.ds(0, 12)], s_sem.at[p, k])
            bytes_wait(held[k][p].at[0], d_sem.at[p, k])
        bytes_wait(cb[p].at[pl.ds(0, 3)], csend_sem.at[p])
        bytes_wait(acc[p].at[pl.ds(0, 3)], rs_send.at[p])


def solution(mesh):
    dev_spec = P(("batch", "k"))

    def per_device(a_loc, b_loc, pair_loc, coord_loc, cidx_loc):
        a, b = a_loc[0], b_loc[0]
        pairs, coords, cidx = (jnp.swapaxes(v[0], -1, -2) for v in (pair_loc, coord_loc, cidx_loc))
        n_own = cidx.shape[1]
        rows, depth, cols = a.shape[1], a.shape[2], b.shape[2]
        assert rows == sum(ROWS)
        f32, i32, bf16 = jnp.float32, jnp.int32, jnp.bfloat16
        dma = pltpu.SemaphoreType.DMA
        out = pl.pallas_call(
            kernel,
            out_shape=jax.ShapeDtypeStruct((n_own, rows, cols), f32),
            in_specs=[pl.BlockSpec(memory_space=pl.ANY)] * 5,
            out_specs=pl.BlockSpec(memory_space=pl.ANY),
            scratch_shapes=[
                pltpu.VMEM(pairs.shape, i32), pltpu.VMEM(coords.shape, i32), pltpu.VMEM(cidx.shape, i32),
                pltpu.VMEM((n_own, rows, cols), f32),
                [pltpu.VMEM((2, LINES, 4, depth, cols), bf16) for cr in ROWS],
                [pltpu.VMEM((2, LINES, 4, cr, depth), bf16) for cr in ROWS],
                [pltpu.VMEM((2, LINES, 2, 8, 128), i32) for cr in ROWS],
                [pltpu.VMEM((NOPAIR + 1, max(ROWS), cols), f32) for _ in range(4)],
                [pltpu.VMEM((NOSLOT + 1, cr, cols), f32) for cr in ROWS],
                [pltpu.VMEM((RING, n_own, cr, cols), f32) for cr in ROWS],
                [pltpu.VMEM((2, n_own // 2, cr, cols), f32) for cr in ROWS],
                [pltpu.VMEM((2, n_own, cr, cols), f32) for cr in ROWS],
                [pltpu.VMEM((RING, 8, 128), i32) for cr in ROWS],
                [pltpu.VMEM((2, 8, 128), i32) for cr in ROWS],
                [pltpu.VMEM((2, n_own, 128), i32) for cr in ROWS],
                [pltpu.SMEM((2, 8, 128), i32) for cr in ROWS],
                [pltpu.SMEM((2, n_own, 128), i32) for cr in ROWS],
                dma((3,)), dma((n_own // GROUP,)), dma((4,)),
                dma((2, 3, LINES, 2)), dma((2, 3, LINES)),
                dma((2, 3)), dma((2, 3)), dma((2, 3)),
                dma((2,)), dma((2, RING)), dma((2,)), dma((2,)),
                dma((2,)), dma((2, 2, n_own // 2 // GROUP)), dma((2, 2, n_own // GROUP)),
            ],
            compiler_params=pltpu.CompilerParams(collective_id=0, has_side_effects=True,
                                                 vmem_limit_bytes=48 * 1024 * 1024),
        )(*[pltpu.with_memory_space_constraint(v, pltpu.HBM) for v in (a, b, pairs, coords, cidx)])
        return out[None]

    return jax.shard_map(per_device, mesh=mesh, in_specs=(dev_spec,) * 5, out_specs=dev_spec, check_vma=False)
```
